32 devices in a mesh: gx: 4 (over y, x), gy: 2 (over core), gz: 4 (over z).
Axes of the slice: x: 2, y: 2, z: 4, core: 2. Of those that a mesh axis runs over, the one named last changes fastest.
Arguments:
- measures: float32 [65536, 256], P(('gx', 'gy', 'gz')), may hold values from -6 to 6
- group_index: int32 [65536], P(('gx', 'gy', 'gz')), may hold values from 0 to 511, as said below
- distinct_keys: int32 [32, 512], P(('gx', 'gy', 'gz')), may hold values from 32 to 65567, as said below
- group_counts: int32 [32], P(('gx', 'gy', 'gz')), may hold values from 128 to 512, as said below
Outputs:
- group_sums: float32 [16384, 256], P(('gx', 'gy', 'gz'))
- group_rows: int32 [16384], P(('gx', 'gy', 'gz'))
- group_keys: int32 [16384], P(('gx', 'gy', 'gz'))
- group_total: int32 [], replicated
The draws below stay inside these ranges and needn't reach their ends.
Inputs may be any that keep to these rules, and one draw needn't show every extreme that they name: `group_counts`: every device has between 128 and 512 groups, and some device has exactly 512. `group_index`: each row's index lies below its device's group count, and every group of a device has at least one row. `distinct_keys`: each device's keys rise strictly; all keys of device d equal d modulo 32, so no key lives on two devices; entries at and past the device's count are unused.
All inputs are finite; a program needn't handle non-finite values.
Results may differ from the reference program's by a relative error of at most 0.0003.
Values sent between devices are 32-bit elements; how exact they have to be, the bound alone decides.
A program may use at most 64 MiB of HBM per device.

```python
import jax
import jax.numpy as jnp
from jax import lax

ROW_DEV = 2048
M = 256
GMAX = 512
ROWS = 65536
DEVICES = 32


def shared_counts(key):
    counts = jax.random.randint(jax.random.fold_in(key, 7), (DEVICES,), GMAX // 4, GMAX + 1)
    fullest = jax.random.randint(jax.random.fold_in(key, 8), (), 0, DEVICES)
    return counts.at[fullest].set(GMAX).astype(jnp.int32)


def draw_group_counts(key, part):
    return shared_counts(key)


def one_device(key, count):
    places = jnp.arange(ROW_DEV, dtype=jnp.int32)
    upper = jnp.minimum(jax.random.randint(jax.random.fold_in(key, 1), (ROW_DEV,), 1, GMAX + 1), count)
    picked = jax.random.randint(jax.random.fold_in(key, 2), (ROW_DEV,), 0, upper)
    picked = jnp.where(places < count, places, picked % count)
    order = jax.random.permutation(jax.random.fold_in(key, 3), ROW_DEV)
    return picked[order].astype(jnp.int32)


def draw_group_index(key, part):
    counts = shared_counts(key)
    device_keys = jax.vmap(lambda d: jax.random.fold_in(jax.random.fold_in(key, 11), d))(jnp.arange(DEVICES))
    return jax.vmap(one_device)(device_keys, counts).reshape(-1)


def draw_distinct_keys(key, part):
    steps = jax.random.randint(jax.random.fold_in(key, 21), (DEVICES, GMAX), 1, 5)
    steps = steps.at[0, 0].set(1)
    rising = jnp.cumsum(steps, axis=1)
    rising = rising.at[:, GMAX - 1].set(4 * GMAX)
    owner = jnp.arange(DEVICES, dtype=jnp.int32)[:, None]
    return (owner + DEVICES * rising).astype(jnp.int32)


def shard_levels(key, extent, pieces, least, top_value):
    loudness = 1.0
    for dim, blocks in pieces:
        draws = jax.random.uniform(jax.random.fold_in(jax.random.fold_in(key, 6), dim), (blocks,), jnp.float32, least / len(pieces), top_value / len(pieces))
        loudness = loudness * jnp.repeat(jnp.exp(draws), extent[dim] // blocks).reshape((-1,) + (1,) * (len(extent) - 1 - dim))
    return loudness


def gaussian(key, dims, width, limit, split=(), held_as=jnp.bfloat16):
    drawn = width * jax.random.normal(key, dims, jnp.float32)
    if split:
        drawn = drawn * shard_levels(key, dims, split, -0.22, 0.18)
    return jnp.clip(drawn, -limit, limit).astype(held_as)


def setup_inputs(seed: int = 0) -> dict:
    arg_keys = jax.random.split(jax.random.key(seed), 5)
    measures = gaussian(arg_keys[0], (ROWS, M), 1.0, 6.0, ((0, 32),), jnp.float32)
    group_index = draw_group_index(jax.random.fold_in(arg_keys[4], 71), 0)
    distinct_keys = draw_distinct_keys(jax.random.fold_in(arg_keys[4], 71), 0)
    group_counts = draw_group_counts(jax.random.fold_in(arg_keys[4], 71), 0)
    return dict(measures=measures, group_index=group_index, distinct_keys=distinct_keys, group_counts=group_counts)


def local_groups(pair):
    values, index = pair
    sums = jax.ops.segment_sum(values, index, num_segments=GMAX)
    rows = jax.ops.segment_sum(jnp.ones_like(index), index, num_segments=GMAX)
    return sums, rows


def reference(measures, group_index, distinct_keys, group_counts):
    offsets = jnp.cumsum(group_counts) - group_counts
    group_total = jnp.sum(group_counts).astype(jnp.int32)
    values = measures.reshape(DEVICES, ROW_DEV, M)
    index = group_index.reshape(DEVICES, ROW_DEV)
    sums, rows = lax.map(local_groups, (values, index))
    local = jnp.arange(GMAX, dtype=jnp.int32)
    dense = offsets[:, None] + local[None, :]
    live = local[None, :] < group_counts[:, None]
    where_to = (dense % DEVICES) * GMAX + dense // DEVICES
    where_to = jnp.where(live, where_to, DEVICES * GMAX).astype(jnp.int32).reshape(-1)
    group_sums = jnp.zeros((DEVICES * GMAX, M), jnp.float32).at[where_to].set(sums.reshape(-1, M), mode="drop")
    group_rows = jnp.zeros((DEVICES * GMAX,), jnp.int32).at[where_to].set(rows.reshape(-1).astype(jnp.int32), mode="drop")
    group_keys = jnp.full((DEVICES * GMAX,), -1, jnp.int32).at[where_to].set(distinct_keys.reshape(-1), mode="drop")
    return group_sums, group_rows, group_keys, group_total
```

```python
import functools

import jax
import jax.numpy as jnp
from jax import lax
from jax.experimental import pallas as pl
from jax.experimental.pallas import tpu as pltpu
from jax.sharding import PartitionSpec as P

AXES = ("gx", "gy", "gz")
LANES = 128
MESH = pl.DeviceIdType.MESH


def round_up(value, unit):
    return (value + unit - 1) // unit * unit


def relative_steps(dims):
    nx, ny, nz = dims
    steps = [(a, b, c) for c in range(nz) for a in range(nx) for b in range(ny)]
    return [k for k in steps if k != (0, 0, 0)]


def wrapped(value, size):
    return jnp.where(value >= size, value - size, value)


def modulo(value, size):
    if size & (size - 1) == 0:
        return value & (size - 1)
    return lax.rem(value, size)


def divide(value, size):
    if size & (size - 1) == 0:
        return lax.shift_right_arithmetic(value, jnp.int32(size.bit_length() - 1))
    return value // size


def flat(spot, dims):
    return (spot[0] * dims[1] + spot[1]) * dims[2] + spot[2]


def targets_of(spots, dims):
    nx, ny, nz = dims
    half = nz // 2 if nz % 2 == 0 else nz
    side = spots[2] // half
    sides = nz // half
    targets = []
    for s in range(1, sides + 1):
        base = wrapped(side + s, sides) * half
        for c in range(half):
            for a in range(nx):
                for b in range(ny):
                    spot = (wrapped(spots[0] + a, nx), wrapped(spots[1] + b, ny), base + c)
                    targets.append((spot, s == sides and a == 0 and b == 0))
    return targets


def exchange_kernel(
    shape,
    index_hbm,
    keys_hbm,
    count_hbm,
    measures_ref,
    recv_ref,
    counts_ref,
    held,
    stage,
    send,
    tally_ref,
    cbuf,
    index_ref,
    keys_ref,
    count_ref,
    small_sem,
    load_sem,
    count_sem,
    data_sem,
):
    dims, span, levels, chunks, fields_at = shape
    nx, ny, nz = dims
    devices = nx * ny * nz
    spots = [lax.axis_index(axis) for axis in AXES]
    me = flat(spots, dims)
    ring = [[wrapped(spot + k, size) for k in range(size)] for spot, size in zip(spots, dims)]
    rows, width = held.shape
    chunk = rows // chunks
    halves = width // LANES
    sent_rows = fields_at + 1
    steps = relative_steps(dims)

    count_load = pltpu.make_async_copy(count_hbm, count_ref, small_sem.at[0])
    count_load.start()
    barrier = pltpu.get_barrier_semaphore()
    for k in steps:
        pl.semaphore_signal(
            barrier, inc=1, device_id=tuple(r[i] for r, i in zip(ring, k)), device_id_type=MESH
        )
    index_load = pltpu.make_async_copy(index_hbm, index_ref, small_sem.at[1])
    index_load.start()
    loads = []
    for c in range(chunks):
        piece = pl.ds(c * chunk, chunk)
        load = pltpu.make_async_copy(measures_ref.at[piece], held.at[piece], load_sem.at[c])
        load.start()
        loads.append(load)
    keys_load = pltpu.make_async_copy(keys_hbm, keys_ref, small_sem.at[2])
    keys_load.start()

    def remote(source, goal, sems, spot):
        return pltpu.make_async_remote_copy(
            src_ref=source,
            dst_ref=goal,
            send_sem=sems.at[0],
            recv_sem=sems.at[1],
            device_id=tuple(spot),
            device_id_type=MESH,
        )

    count_load.wait()
    cbuf[me] = jnp.full(cbuf.shape[1:], count_ref[0], jnp.int32)
    index_load.wait()

    row = lax.broadcasted_iota(jnp.int32, (span, LANES), 0)
    labels = lax.rem(row, levels) * devices + row // levels

    for c in range(chunks):
        loads[c].wait()
        x = held[pl.ds(c * chunk, chunk), :]
        high = x.astype(jnp.bfloat16)
        low = (x - high.astype(jnp.float32)).astype(jnp.bfloat16)
        parts = []
        for j in range(chunk // LANES):
            at = c * (chunk // LANES) + j
            hit = jnp.where(index_ref[pl.ds(at, 1), :] == labels, 1.0, 0.0)
            if at == 0:
                tally_ref[...] = hit
            else:
                tally_ref[...] += hit
            parts.append(hit.astype(jnp.bfloat16))
        hits = jnp.concatenate(parts, axis=1)
        dot = functools.partial(jnp.dot, preferred_element_type=jnp.float32)
        part = dot(hits, high) + dot(hits, low)
        for h in range(halves):
            block = part[:, h * LANES : (h + 1) * LANES].reshape(devices, levels, LANES)
            if c == 0:
                stage[:, h * levels : (h + 1) * levels, :] = block
            else:
                stage[:, h * levels : (h + 1) * levels, :] += block
        if c == 0:
            pl.semaphore_wait(barrier, devices - 1)
            for k in steps:
                remote(cbuf.at[me], cbuf.at[me], count_sem, [r[i] for r, i in zip(ring, k)]).start()

    tallies = lax.dot_general(
        jnp.ones((8, LANES), jnp.bfloat16),
        tally_ref[...].astype(jnp.bfloat16),
        (((1,), (1,)), ((), ())),
        preferred_element_type=jnp.float32,
    )
    keys_load.wait()
    keys = keys_ref[...]
    source = lax.broadcasted_iota(jnp.int32, (span, span), 0)
    goal = lax.broadcasted_iota(jnp.int32, (span, span), 1)
    moved = (source == lax.rem(goal, levels) * devices + goal // levels)
    moved = jnp.where(moved, 1.0, 0.0).astype(jnp.bfloat16)
    line = lax.broadcasted_iota(jnp.int32, (8, span), 0)
    pieces = jnp.where(
        line == 0, keys & 255, jnp.where(line == 1, (keys >> 8) & 255, (keys >> 16) & 255)
    )
    pieces = jnp.dot(
        pieces.astype(jnp.float32).astype(jnp.bfloat16), moved, preferred_element_type=jnp.float32
    )
    placed = pieces[0:1] + pieces[1:2] * 256.0 + pieces[2:3] * 65536.0
    lane = lax.broadcasted_iota(jnp.int32, (1, LANES), 1)
    for t in range(span // LANES):
        tile = slice(t * LANES, (t + 1) * LANES)
        keyed = pltpu.roll(jnp.broadcast_to(placed[:, tile], (8, LANES)), LANES // 2, 1)[0:1]
        counted = tallies[0:1, tile]
        lows = jnp.where(lane < LANES // 2, counted, keyed)
        highs = jnp.where(lane < LANES // 2, keyed, counted)
        for a in range(t * LANES // levels, (t + 1) * LANES // levels):
            within = a * levels % LANES
            stage[a, fields_at : fields_at + 1, :] = lows if within < LANES // 2 else highs

    others = cbuf.at[pl.ds(1, devices - 1)]
    pltpu.make_async_copy(others, others, count_sem.at[1]).wait()
    counts = cbuf[...][:, 0, :]
    sender = lax.broadcasted_iota(jnp.int32, counts.shape, 0)
    place = lax.broadcasted_iota(jnp.int32, counts.shape, 1)
    before = jnp.sum(jnp.where(sender < me, counts, 0), axis=0, keepdims=True)[0, 0]
    shift = modulo(before, devices)

    targets = targets_of(spots, dims)
    for spot, _ in targets:
        other = flat(spot, dims)
        send[other] = stage[modulo(other - shift + devices, devices)]
    piece = pl.ds(0, sent_rows)
    for spot, maybe in targets:
        other = flat(spot, dims)
        copy = remote(send.at[other, piece], recv_ref.at[me, piece], data_sem, spot)
        if maybe:
            pl.when(other != me)(copy.start)
        else:
            copy.start()
    recv_ref[me] = send[me]
    counts_ref[...] = jnp.sum(jnp.where(sender == place, counts, 0), axis=0, keepdims=True)
    pltpu.make_async_copy(others, others, count_sem.at[0]).wait()
    landed = recv_ref.at[pl.ds(1, devices - 1), pl.ds(0, sent_rows)]
    left = send.at[pl.ds(1, devices - 1), pl.ds(0, sent_rows)]
    pltpu.make_async_copy(left, left, data_sem.at[0]).wait()
    pltpu.make_async_copy(landed, landed, data_sem.at[1]).wait()


def place_kernel(
    shape, counts_ref, recv_ref, sums_ref, rows_ref, keys_ref, total_ref, buf
):
    dims, span, levels, fields_at = shape
    nx, ny, nz = dims
    devices = nx * ny * nz
    spots = [lax.axis_index(axis) for axis in AXES]
    me = (spots[0] * ny + spots[1]) * nz + spots[2]
    halves = sums_ref.shape[1] // LANES
    lane = lax.broadcasted_iota(jnp.int32, (8, span), 1)
    fields = jnp.zeros((8, span), jnp.float32)
    keyed = fields
    offset = jnp.int32(0)

    for d in range(devices):
        first = modulo(me - modulo(offset, devices) + devices, devices)
        start = divide(offset + first, devices)
        for h in range(halves):
            buf[h, pl.ds(start, levels), :] = recv_ref[d, h * levels : (h + 1) * levels, :]
        turn = modulo(modulo(start, LANES) - modulo(first * levels, LANES) + LANES, LANES)
        turned = pltpu.roll(recv_ref[d, fields_at : fields_at + 8, :], turn, 1)
        wide = jnp.concatenate([turned] * (span // LANES), axis=1)
        fields = jnp.where(lane >= start, wide, fields)
        turned = pltpu.roll(turned, LANES // 2, 1)
        wide = jnp.concatenate([turned] * (span // LANES), axis=1)
        keyed = jnp.where(lane >= start, wide, keyed)
        offset = offset + counts_ref[0, d]

    total_ref[0, 0] = offset
    taken = divide(offset - me + devices - 1, devices)
    row = lax.broadcasted_iota(jnp.int32, (span, LANES), 0)
    for h in range(halves):
        sums_ref[:, h * LANES : (h + 1) * LANES] = jnp.where(row < taken, buf[h, 0:span, :], 0.0)
    inside = lane[0:1] < taken
    rows_ref[...] = jnp.where(inside, fields[0:1].astype(jnp.int32), 0)
    keys_ref[...] = jnp.where(inside, keyed[0:1].astype(jnp.int32), -1)


def shards(measures, group_index, distinct_keys, group_counts):
    rows, width = measures.shape
    span = distinct_keys.shape[1]
    dims = tuple(lax.axis_size(axis) for axis in AXES)
    devices = dims[0] * dims[1] * dims[2]
    levels = span // devices
    chunks = 4 if rows % (4 * LANES) == 0 else 1
    fields_at = levels * (width // LANES)
    slab = round_up(fields_at + 8, 8)
    wide = round_up(devices, LANES)
    vmem = pl.BlockSpec(memory_space=pltpu.VMEM)
    smem = pl.BlockSpec(memory_space=pltpu.SMEM)
    anywhere = pl.BlockSpec(memory_space=pl.ANY)
    received, counts = pl.pallas_call(
        functools.partial(
            exchange_kernel, (dims, span, levels, chunks, fields_at)
        ),
        out_shape=(
            pltpu.VMEM((devices, slab, LANES), jnp.float32),
            pltpu.VMEM((1, wide), jnp.int32),
        ),
        in_specs=[anywhere] * 4,
        out_specs=(vmem, vmem),
        scratch_shapes=[
            pltpu.VMEM((rows, width), jnp.float32),
            pltpu.VMEM((devices, slab, LANES), jnp.float32),
            pltpu.VMEM((devices, slab, LANES), jnp.float32),
            pltpu.VMEM((span, LANES), jnp.float32),
            pltpu.VMEM((devices, 1, wide), jnp.int32),
            pltpu.VMEM((rows // LANES, LANES), jnp.int32),
            pltpu.VMEM((1, span), jnp.int32),
            pltpu.SMEM((1,), jnp.int32),
            pltpu.SemaphoreType.DMA((3,)),
            pltpu.SemaphoreType.DMA((chunks,)),
            pltpu.SemaphoreType.DMA((2,)),
            pltpu.SemaphoreType.DMA((2,)),
        ],
        compiler_params=pltpu.CompilerParams(collective_id=0, has_side_effects=True),
        name="exchange",
    )(group_index.reshape(rows // LANES, LANES), distinct_keys, group_counts, measures)
    sums, tallies, keys, total = pl.pallas_call(
        functools.partial(place_kernel, (dims, span, levels, fields_at)),
        out_shape=(
            jax.ShapeDtypeStruct((span, width), jnp.float32),
            jax.ShapeDtypeStruct((1, span), jnp.int32),
            jax.ShapeDtypeStruct((1, span), jnp.int32),
            jax.ShapeDtypeStruct((1, 1), jnp.int32),
        ),
        in_specs=[smem, vmem],
        out_specs=(vmem, vmem, vmem, smem),
        scratch_shapes=[pltpu.VMEM((width // LANES, span + round_up(levels, 8), LANES), jnp.float32)],
        compiler_params=pltpu.CompilerParams(vmem_limit_bytes=16 * 1024 * 1024),
        name="place",
    )(*(pltpu.with_memory_space_constraint(part, pltpu.VMEM) for part in (counts, received)))
    return sums, tallies.reshape(span), keys.reshape(span), total.reshape(())


def solution(mesh):
    return jax.shard_map(
        shards,
        mesh=mesh,
        in_specs=(
            P(AXES, None),
            P(AXES),
            P(AXES, None),
            P(AXES),
        ),
        out_specs=(P(AXES, None), P(AXES), P(AXES), P()),
        check_vma=False,
    )
```

```python
import functools

import jax
import jax.numpy as jnp
from jax import lax
from jax.experimental import pallas as pl
from jax.experimental.pallas import tpu as pltpu
from jax.sharding import PartitionSpec as P

AXES = ("gx", "gy", "gz")
LANES = 128
MESH = pl.DeviceIdType.MESH


def round_up(value, unit):
    return (value + unit - 1) // unit * unit


def wrapped(value, size):
    return jnp.where(value >= size, value - size, value)


def modulo(value, size):
    if size & (size - 1) == 0:
        return value & (size - 1)
    return lax.rem(value, size)


def divide(value, size):
    if size & (size - 1) == 0:
        return lax.shift_right_arithmetic(value, jnp.int32(size.bit_length() - 1))
    return value // size


def flat(spot, dims):
    return (spot[0] * dims[1] + spot[1]) * dims[2] + spot[2]


def targets_of(spots, dims):
    nx, ny, nz = dims
    half = nz // 2 if nz % 2 == 0 else nz
    side = spots[2] // half
    sides = nz // half
    targets = []
    for s in range(1, sides + 1):
        base = wrapped(side + s, sides) * half
        for c in range(half):
            for a in range(nx):
                for b in range(ny):
                    spot = (wrapped(spots[0] + a, nx), wrapped(spots[1] + b, ny), base + c)
                    targets.append((spot, s == sides and a == 0 and b == 0))
    return targets


def exchange_kernel(
    shape,
    index_hbm,
    keys_hbm,
    measures_ref,
    recv_ref,
    counts_ref,
    held,
    stage,
    send,
    tally_ref,
    cbuf,
    index_ref,
    keys_ref,
    mate_ref,
    small_sem,
    load_sem,
    count_sem,
    data_sem,
):
    dims, span, levels, chunks, fields_at = shape
    nx, ny, nz = dims
    devices = nx * ny * nz
    spots = [lax.axis_index(axis) for axis in AXES]
    me = flat(spots, dims)
    ring = [[wrapped(spot + k, size) for k in range(size)] for spot, size in zip(spots, dims)]
    rows, width = held.shape
    chunk = rows // chunks
    halves = width // LANES
    sent_rows = fields_at + 1

    index_load = pltpu.make_async_copy(index_hbm, index_ref, small_sem.at[1])
    index_load.start()
    cores = 2 if ny % 2 == 0 else 1
    core = modulo(spots[1], cores)
    leads = core == cores - 1
    pairs = ny // cores
    chips = nx * pairs * nz
    pair = divide(spots[1], cores)
    chip = (spots[0] * pairs + pair) * nz + spots[2]
    mate = (spots[0], spots[1] + 1 - 2 * core, spots[2])
    leaders, followers = [], []
    for a in range(nx):
        for b in range(pairs):
            for c in range(nz):
                spot = [ring[0][a], wrapped(pair + b, pairs) * cores, ring[2][c]]
                if (a, b, c) != (0, 0, 0):
                    leaders.append((spot[0], spot[1] + cores - 1, spot[2]))
                    if cores == 2:
                        followers.append(tuple(spot))

    barrier = pltpu.get_barrier_semaphore()
    if cores == 2:
        pl.semaphore_signal(barrier, inc=1, device_id=mate, device_id_type=MESH)
    for spot in leaders:
        pl.semaphore_signal(barrier, inc=1, device_id=spot, device_id_type=MESH)
    loads = []
    for c in range(chunks):
        piece = pl.ds(c * chunk, chunk)
        load = pltpu.make_async_copy(measures_ref.at[piece], held.at[piece], load_sem.at[c])
        load.start()
        loads.append(load)
    keys_load = pltpu.make_async_copy(keys_hbm, keys_ref, small_sem.at[2])
    keys_load.start()

    def remote(source, goal, sems, spot):
        return pltpu.make_async_remote_copy(
            src_ref=source,
            dst_ref=goal,
            send_sem=sems.at[0],
            recv_sem=sems.at[1],
            device_id=tuple(spot),
            device_id_type=MESH,
        )

    index_load.wait()
    top = jnp.max(index_ref[...], axis=0, keepdims=True)
    mine = jnp.broadcast_to(jnp.max(top, axis=1, keepdims=True) + 1, cbuf.shape[1:])
    lane = lax.broadcasted_iota(jnp.int32, cbuf.shape[1:], 1)
    wide_chip = divide(lane, cores * nz) * nz + modulo(lane, nz)
    wide_core = modulo(divide(lane, nz), cores)
    cbuf[chip] = mine

    def tell_mate():
        pl.semaphore_wait(barrier, 1)
        mate_copy.start()

    def tell_all():
        pl.semaphore_wait(barrier, devices - 1)
        if cores == 2:
            mate_copy.wait_recv()
            cbuf[chip] = jnp.where(wide_core == core, mine, mate_ref[1])
            remote(cbuf.at[chip], cbuf.at[chip], count_sem, mate).start()
        for spot in leaders + followers:
            remote(cbuf.at[chip], cbuf.at[chip], count_sem, spot).start()

    if cores == 2:
        mate_ref[0] = mine
        mate_copy = pltpu.make_async_remote_copy(
            src_ref=mate_ref.at[0],
            dst_ref=mate_ref.at[1],
            send_sem=small_sem.at[0],
            recv_sem=small_sem.at[3],
            device_id=mate,
            device_id_type=MESH,
        )
        pl.when(jnp.logical_not(leads))(tell_mate)

    row = lax.broadcasted_iota(jnp.int32, (span, LANES), 0)
    labels = lax.rem(row, levels) * devices + row // levels

    for c in range(chunks):
        loads[c].wait()
        x = held[pl.ds(c * chunk, chunk), :]
        high = x.astype(jnp.bfloat16)
        low = (x - high.astype(jnp.float32)).astype(jnp.bfloat16)
        parts = []
        for j in range(chunk // LANES):
            at = c * (chunk // LANES) + j
            hit = jnp.where(index_ref[pl.ds(at, 1), :] == labels, 1.0, 0.0)
            if at == 0:
                tally_ref[...] = hit
            else:
                tally_ref[...] += hit
            parts.append(hit.astype(jnp.bfloat16))
        hits = jnp.concatenate(parts, axis=1)
        dot = functools.partial(jnp.dot, preferred_element_type=jnp.float32)
        part = dot(hits, high) + dot(hits, low)
        for h in range(halves):
            block = part[:, h * LANES : (h + 1) * LANES].reshape(devices, levels, LANES)
            if c == 0:
                stage[:, h * levels : (h + 1) * levels, :] = block
            else:
                stage[:, h * levels : (h + 1) * levels, :] += block
        if c == 0:
            pl.when(leads)(tell_all)

    tallies = lax.dot_general(
        jnp.ones((8, LANES), jnp.bfloat16),
        tally_ref[...].astype(jnp.bfloat16),
        (((1,), (1,)), ((), ())),
        preferred_element_type=jnp.float32,
    )
    keys_load.wait()
    keys = keys_ref[...]
    source = lax.broadcasted_iota(jnp.int32, (span, span), 0)
    goal = lax.broadcasted_iota(jnp.int32, (span, span), 1)
    moved = (source == lax.rem(goal, levels) * devices + goal // levels)
    moved = jnp.where(moved, 1.0, 0.0).astype(jnp.bfloat16)
    line = lax.broadcasted_iota(jnp.int32, (8, span), 0)
    pieces = jnp.where(
        line == 0, keys & 255, jnp.where(line == 1, (keys >> 8) & 255, (keys >> 16) & 255)
    )
    pieces = jnp.dot(
        pieces.astype(jnp.float32).astype(jnp.bfloat16), moved, preferred_element_type=jnp.float32
    )
    placed = pieces[0:1] + pieces[1:2] * 256.0 + pieces[2:3] * 65536.0
    line = lax.broadcasted_iota(jnp.int32, (1, LANES), 1)
    for t in range(span // LANES):
        tile = slice(t * LANES, (t + 1) * LANES)
        keyed = pltpu.roll(jnp.broadcast_to(placed[:, tile], (8, LANES)), LANES // 2, 1)[0:1]
        counted = tallies[0:1, tile]
        lows = jnp.where(line < LANES // 2, counted, keyed)
        highs = jnp.where(line < LANES // 2, keyed, counted)
        for a in range(t * LANES // levels, (t + 1) * LANES // levels):
            within = a * levels % LANES
            stage[a, fields_at : fields_at + 1, :] = lows if within < LANES // 2 else highs

    def await_others():
        others = cbuf.at[pl.ds(1, chips - 1)]
        pltpu.make_async_copy(others, others, count_sem.at[1]).wait()

    def await_all():
        pltpu.make_async_copy(cbuf, cbuf, count_sem.at[1]).wait()

    pl.when(leads)(await_others)
    if cores == 2:
        pl.when(jnp.logical_not(leads))(await_all)
    shown = cbuf[...][:, 0, :]
    place = lax.broadcasted_iota(jnp.int32, shown.shape, 0)
    counts = jnp.sum(jnp.where(place == wide_chip, shown, 0), axis=0, keepdims=True)
    before = jnp.sum(jnp.where(lane < me, counts, 0))
    shift = modulo(before, devices)

    targets = targets_of(spots, dims)
    for spot, _ in targets:
        other = flat(spot, dims)
        send[other] = stage[modulo(other - shift + devices, devices)]
    piece = pl.ds(0, sent_rows)
    for spot, maybe in targets:
        other = flat(spot, dims)
        copy = remote(send.at[other, piece], recv_ref.at[me, piece], data_sem, spot)
        if maybe:
            pl.when(other != me)(copy.start)
        else:
            copy.start()
    recv_ref[me] = send[me]
    counts_ref[...] = counts

    def sent_counts():
        told = cbuf.at[pl.ds(1, chips - 1)]
        pltpu.make_async_copy(told, told, count_sem.at[0]).wait()
        if cores == 2:
            pltpu.make_async_copy(cbuf, cbuf, count_sem.at[0]).wait()

    pl.when(leads)(sent_counts)
    if cores == 2:
        pl.when(jnp.logical_not(leads))(mate_copy.wait_send)
    landed = recv_ref.at[pl.ds(1, devices - 1), pl.ds(0, sent_rows)]
    left = send.at[pl.ds(1, devices - 1), pl.ds(0, sent_rows)]
    pltpu.make_async_copy(left, left, data_sem.at[0]).wait()
    pltpu.make_async_copy(landed, landed, data_sem.at[1]).wait()


def place_kernel(
    shape, counts_ref, recv_ref, sums_ref, rows_ref, keys_ref, total_ref, buf
):
    dims, span, levels, fields_at = shape
    nx, ny, nz = dims
    devices = nx * ny * nz
    spots = [lax.axis_index(axis) for axis in AXES]
    me = (spots[0] * ny + spots[1]) * nz + spots[2]
    halves = sums_ref.shape[1] // LANES
    lane = lax.broadcasted_iota(jnp.int32, (8, span), 1)
    fields = jnp.zeros((8, span), jnp.float32)
    keyed = fields
    offset = jnp.int32(0)

    for d in range(devices):
        first = modulo(me - modulo(offset, devices) + devices, devices)
        start = divide(offset + first, devices)
        for h in range(halves):
            buf[h, pl.ds(start, levels), :] = recv_ref[d, h * levels : (h + 1) * levels, :]
        turn = modulo(modulo(start, LANES) - modulo(first * levels, LANES) + LANES, LANES)
        turned = pltpu.roll(recv_ref[d, fields_at : fields_at + 8, :], turn, 1)
        wide = jnp.concatenate([turned] * (span // LANES), axis=1)
        fields = jnp.where(lane >= start, wide, fields)
        turned = pltpu.roll(turned, LANES // 2, 1)
        wide = jnp.concatenate([turned] * (span // LANES), axis=1)
        keyed = jnp.where(lane >= start, wide, keyed)
        offset = offset + counts_ref[0, d]

    total_ref[0, 0] = offset
    taken = divide(offset - me + devices - 1, devices)
    row = lax.broadcasted_iota(jnp.int32, (span, LANES), 0)
    for h in range(halves):
        sums_ref[:, h * LANES : (h + 1) * LANES] = jnp.where(row < taken, buf[h, 0:span, :], 0.0)
    inside = lane[0:1] < taken
    rows_ref[...] = jnp.where(inside, fields[0:1].astype(jnp.int32), 0)
    keys_ref[...] = jnp.where(inside, keyed[0:1].astype(jnp.int32), -1)


def shards(measures, group_index, distinct_keys, group_counts):
    rows, width = measures.shape
    span = distinct_keys.shape[1]
    dims = tuple(lax.axis_size(axis) for axis in AXES)
    devices = dims[0] * dims[1] * dims[2]
    levels = span // devices
    chunks = 4 if rows % (4 * LANES) == 0 else 1
    fields_at = levels * (width // LANES)
    slab = round_up(fields_at + 8, 8)
    wide = round_up(devices, LANES)
    cores = 2 if dims[1] % 2 == 0 else 1
    vmem = pl.BlockSpec(memory_space=pltpu.VMEM)
    smem = pl.BlockSpec(memory_space=pltpu.SMEM)
    anywhere = pl.BlockSpec(memory_space=pl.ANY)
    received, counts = pl.pallas_call(
        functools.partial(
            exchange_kernel, (dims, span, levels, chunks, fields_at)
        ),
        out_shape=(
            pltpu.VMEM((devices, slab, LANES), jnp.float32),
            pltpu.VMEM((1, wide), jnp.int32),
        ),
        in_specs=[anywhere] * 3,
        out_specs=(vmem, vmem),
        scratch_shapes=[
            pltpu.VMEM((rows, width), jnp.float32),
            pltpu.VMEM((devices, slab, LANES), jnp.float32),
            pltpu.VMEM((devices, slab, LANES), jnp.float32),
            pltpu.VMEM((span, LANES), jnp.float32),
            pltpu.VMEM((devices // cores, 1, wide), jnp.int32),
            pltpu.VMEM((rows // LANES, LANES), jnp.int32),
            pltpu.VMEM((1, span), jnp.int32),
            pltpu.VMEM((2, 1, wide), jnp.int32),
            pltpu.SemaphoreType.DMA((4,)),
            pltpu.SemaphoreType.DMA((chunks,)),
            pltpu.SemaphoreType.DMA((2,)),
            pltpu.SemaphoreType.DMA((2,)),
        ],
        compiler_params=pltpu.CompilerParams(collective_id=0, has_side_effects=True),
        name="exchange",
    )(group_index.reshape(rows // LANES, LANES), distinct_keys, measures)
    sums, tallies, keys, total = pl.pallas_call(
        functools.partial(place_kernel, (dims, span, levels, fields_at)),
        out_shape=(
            jax.ShapeDtypeStruct((span, width), jnp.float32),
            jax.ShapeDtypeStruct((1, span), jnp.int32),
            jax.ShapeDtypeStruct((1, span), jnp.int32),
            jax.ShapeDtypeStruct((1, 1), jnp.int32),
        ),
        in_specs=[smem, vmem],
        out_specs=(vmem, vmem, vmem, smem),
        scratch_shapes=[pltpu.VMEM((width // LANES, span + round_up(levels, 8), LANES), jnp.float32)],
        compiler_params=pltpu.CompilerParams(vmem_limit_bytes=16 * 1024 * 1024),
        name="place",
    )(*(pltpu.with_memory_space_constraint(part, pltpu.VMEM) for part in (counts, received)))
    return sums, tallies.reshape(span), keys.reshape(span), total.reshape(())


def solution(mesh):
    return jax.shard_map(
        shards,
        mesh=mesh,
        in_specs=(
            P(AXES, None),
            P(AXES),
            P(AXES, None),
            P(AXES),
        ),
        out_specs=(P(AXES, None), P(AXES), P(AXES), P()),
        check_vma=False,
    )
```

```python
import functools

import jax
import jax.numpy as jnp
from jax import lax
from jax.experimental import pallas as pl
from jax.experimental.pallas import tpu as pltpu
from jax.sharding import PartitionSpec as P

AXES = ("gx", "gy", "gz")
LANES = 128
MESH = pl.DeviceIdType.MESH


def round_up(value, unit):
    return (value + unit - 1) // unit * unit


def wrapped(value, size):
    return jnp.where(value >= size, value - size, value)


def modulo(value, size):
    if size & (size - 1) == 0:
        return value & (size - 1)
    return lax.rem(value, size)


def divide(value, size):
    if size & (size - 1) == 0:
        return lax.shift_right_arithmetic(value, jnp.int32(size.bit_length() - 1))
    return value // size


def flat(spot, dims):
    return (spot[0] * dims[1] + spot[1]) * dims[2] + spot[2]


def targets_of(spots, dims):
    nx, ny, nz = dims
    half = nz // 2 if nz % 2 == 0 else nz
    sides = nz // half
    side = spots[2] // half
    targets = []
    for s in range(1, sides + 1):
        base = wrapped(side + s, sides) * half
        for c in range(half):
            for a in range(nx):
                for b in range(ny):
                    targets.append(((jnp.int32(a), jnp.int32(b), base + c), s == sides))
    return targets


def exchange_kernel(
    shape,
    index_hbm,
    keys_hbm,
    measures_ref,
    recv_ref,
    counts_ref,
    held,
    stage,
    send,
    tally_ref,
    cbuf,
    index_ref,
    keys_ref,
    mate_ref,
    counts_kept,
    small_sem,
    load_sem,
    count_sem,
    data_sem,
):
    dims, span, levels, chunks, fields_at = shape
    nx, ny, nz = dims
    devices = nx * ny * nz
    spots = [lax.axis_index(axis) for axis in AXES]
    me = flat(spots, dims)
    ring = [[wrapped(spot + k, size) for k in range(size)] for spot, size in zip(spots, dims)]
    rows, width = held.shape
    chunk = rows // chunks
    halves = width // LANES
    sent_rows = fields_at + 1

    index_load = pltpu.make_async_copy(index_hbm, index_ref, small_sem.at[1])
    index_load.start()
    cores = 2 if ny % 2 == 0 else 1
    core = modulo(spots[1], cores)
    leads = core == cores - 1
    pairs = ny // cores
    chips = nx * pairs * nz
    pair = divide(spots[1], cores)
    chip = (spots[0] * pairs + pair) * nz + spots[2]
    mate = (spots[0], spots[1] + 1 - 2 * core, spots[2])
    leaders, followers = [], []
    for a in range(nx):
        for b in range(pairs):
            for c in range(nz):
                spot = [ring[0][a], wrapped(pair + b, pairs) * cores, ring[2][c]]
                if (a, b, c) != (0, 0, 0):
                    leaders.append((spot[0], spot[1] + cores - 1, spot[2]))
                    if cores == 2:
                        followers.append(tuple(spot))

    barrier = pltpu.get_barrier_semaphore()
    if cores == 2:
        pl.semaphore_signal(barrier, inc=1, device_id=mate, device_id_type=MESH)
    for spot in leaders:
        pl.semaphore_signal(barrier, inc=1, device_id=spot, device_id_type=MESH)
    loads = []
    for c in range(chunks):
        piece = pl.ds(c * chunk, chunk)
        load = pltpu.make_async_copy(measures_ref.at[piece], held.at[piece], load_sem.at[c])
        load.start()
        loads.append(load)
    keys_load = pltpu.make_async_copy(keys_hbm, keys_ref, small_sem.at[2])
    keys_load.start()

    def remote(source, goal, sems, spot):
        return pltpu.make_async_remote_copy(
            src_ref=source,
            dst_ref=goal,
            send_sem=sems.at[0],
            recv_sem=sems.at[1],
            device_id=tuple(spot),
            device_id_type=MESH,
        )

    index_load.wait()
    top = jnp.max(index_ref[...], axis=0, keepdims=True)
    mine = jnp.broadcast_to(jnp.max(top, axis=1, keepdims=True) + 1, cbuf.shape[1:])
    lane = lax.broadcasted_iota(jnp.int32, cbuf.shape[1:], 1)
    wide_chip = divide(lane, cores * nz) * nz + modulo(lane, nz)
    wide_core = modulo(divide(lane, nz), cores)
    cbuf[chip] = mine

    def tell_mate():
        pl.semaphore_wait(barrier, 1)
        mate_copy.start()

    def tell_all():
        pl.semaphore_wait(barrier, devices - 1)
        if cores == 2:
            mate_copy.wait_recv()
            cbuf[chip] = jnp.where(wide_core == core, mine, mate_ref[1])
            remote(cbuf.at[chip], cbuf.at[chip], count_sem, mate).start()
        for spot in leaders + followers:
            remote(cbuf.at[chip], cbuf.at[chip], count_sem, spot).start()

    if cores == 2:
        mate_ref[0] = mine
        mate_copy = pltpu.make_async_remote_copy(
            src_ref=mate_ref.at[0],
            dst_ref=mate_ref.at[1],
            send_sem=small_sem.at[0],
            recv_sem=small_sem.at[3],
            device_id=mate,
            device_id_type=MESH,
        )
        pl.when(jnp.logical_not(leads))(tell_mate)

    row = lax.broadcasted_iota(jnp.int32, (span, LANES), 0)
    labels = lax.rem(row, levels) * devices + row // levels

    for c in range(chunks):
        loads[c].wait()
        x = held[pl.ds(c * chunk, chunk), :]
        high = x.astype(jnp.bfloat16)
        low = (x - high.astype(jnp.float32)).astype(jnp.bfloat16)
        parts = []
        for j in range(chunk // LANES):
            at = c * (chunk // LANES) + j
            hit = jnp.where(index_ref[pl.ds(at, 1), :] == labels, 1.0, 0.0)
            if at == 0:
                tally_ref[...] = hit
            else:
                tally_ref[...] += hit
            parts.append(hit.astype(jnp.bfloat16))
        hits = jnp.concatenate(parts, axis=1)
        dot = functools.partial(jnp.dot, preferred_element_type=jnp.float32)
        part = dot(hits, high) + dot(hits, low)
        for h in range(halves):
            block = part[:, h * LANES : (h + 1) * LANES].reshape(devices, levels, LANES)
            if c == 0:
                stage[:, h * levels : (h + 1) * levels, :] = block
            else:
                stage[:, h * levels : (h + 1) * levels, :] += block
        if c == 0:
            pl.when(leads)(tell_all)

    tallies = lax.dot_general(
        jnp.ones((8, LANES), jnp.bfloat16),
        tally_ref[...].astype(jnp.bfloat16),
        (((1,), (1,)), ((), ())),
        preferred_element_type=jnp.float32,
    )
    keys_load.wait()
    keys = keys_ref[...]
    source = lax.broadcasted_iota(jnp.int32, (span, span), 0)
    goal = lax.broadcasted_iota(jnp.int32, (span, span), 1)
    moved = (source == lax.rem(goal, levels) * devices + goal // levels)
    moved = jnp.where(moved, 1.0, 0.0).astype(jnp.bfloat16)
    line = lax.broadcasted_iota(jnp.int32, (8, span), 0)
    pieces = jnp.where(
        line == 0, keys & 255, jnp.where(line == 1, (keys >> 8) & 255, (keys >> 16) & 255)
    )
    pieces = jnp.dot(
        pieces.astype(jnp.float32).astype(jnp.bfloat16), moved, preferred_element_type=jnp.float32
    )
    placed = pieces[0:1] + pieces[1:2] * 256.0 + pieces[2:3] * 65536.0
    line = lax.broadcasted_iota(jnp.int32, (1, LANES), 1)
    for t in range(span // LANES):
        tile = slice(t * LANES, (t + 1) * LANES)
        keyed = pltpu.roll(jnp.broadcast_to(placed[:, tile], (8, LANES)), LANES // 2, 1)[0:1]
        counted = tallies[0:1, tile]
        lows = jnp.where(line < LANES // 2, counted, keyed)
        highs = jnp.where(line < LANES // 2, keyed, counted)
        for a in range(t * LANES // levels, (t + 1) * LANES // levels):
            within = a * levels % LANES
            stage[a, fields_at : fields_at + 1, :] = lows if within < LANES // 2 else highs

    def await_others():
        others = cbuf.at[pl.ds(1, chips - 1)]
        pltpu.make_async_copy(others, others, count_sem.at[1]).wait()

    def await_all():
        pltpu.make_async_copy(cbuf, cbuf, count_sem.at[1]).wait()

    pl.when(leads)(await_others)
    if cores == 2:
        pl.when(jnp.logical_not(leads))(await_all)
    shown = cbuf[...][:, 0, :]
    place = lax.broadcasted_iota(jnp.int32, shown.shape, 0)
    counts = jnp.sum(jnp.where(place == wide_chip, shown, 0), axis=0, keepdims=True)
    before = jnp.sum(jnp.where(lane < me, counts, 0))
    shift = modulo(before, devices)

    targets = targets_of(spots, dims)
    piece = pl.ds(0, sent_rows)
    for across in (False, True) if any(not own for _, own in targets) else (True,):
        for spot, own in targets:
            if own == across:
                other = flat(spot, dims)
                send[other] = stage[modulo(other - shift + devices, devices)]
        for spot, own in targets:
            if own == across:
                other = flat(spot, dims)
                copy = remote(send.at[other, piece], recv_ref.at[me, piece], data_sem, spot)
                if own:
                    pl.when(other != me)(copy.start)
                else:
                    copy.start()
    recv_ref[me] = send[me]
    counts_kept[...] = counts
    counts_copy = pltpu.make_async_copy(counts_kept, counts_ref, small_sem.at[4])
    counts_copy.start()

    def sent_counts():
        told = cbuf.at[pl.ds(1, chips - 1)]
        pltpu.make_async_copy(told, told, count_sem.at[0]).wait()
        if cores == 2:
            pltpu.make_async_copy(cbuf, cbuf, count_sem.at[0]).wait()

    pl.when(leads)(sent_counts)
    if cores == 2:
        pl.when(jnp.logical_not(leads))(mate_copy.wait_send)
    landed = recv_ref.at[pl.ds(1, devices - 1), pl.ds(0, sent_rows)]
    left = send.at[pl.ds(1, devices - 1), pl.ds(0, sent_rows)]
    pltpu.make_async_copy(left, left, data_sem.at[0]).wait()
    pltpu.make_async_copy(landed, landed, data_sem.at[1]).wait()
    counts_copy.wait()


def place_kernel(
    shape,
    counts_ref,
    recv_ref,
    sums_ref,
    rows_ref,
    keys_ref,
    total_ref,
    buf,
    row_line,
    key_line,
    total_line,
    sems,
):
    dims, span, levels, fields_at = shape
    nx, ny, nz = dims
    devices = nx * ny * nz
    spots = [lax.axis_index(axis) for axis in AXES]
    me = flat(spots, dims)
    halves = buf.shape[0]

    for h in range(halves):
        buf[h] = jnp.zeros(buf.shape[1:], jnp.float32)
    offset = jnp.int32(0)
    starts, turns = [], []
    for d in range(devices):
        first = modulo(me - modulo(offset, devices) + devices, devices)
        start = divide(offset + first, devices)
        for h in range(halves):
            buf[h, pl.ds(start, levels), :] = recv_ref[d, h * levels : (h + 1) * levels, :]
        starts.append(start)
        turns.append(modulo(start - first * levels + span, LANES))
        offset = offset + counts_ref[0, d]
    copies = []
    for h in range(halves):
        copies.append(
            pltpu.make_async_copy(
                buf.at[h, pl.ds(0, span)], sums_ref.at[:, pl.ds(h * LANES, LANES)], sems.at[h]
            )
        )
        copies[-1].start()

    total_line[0, 0] = offset
    copies.append(pltpu.make_async_copy(total_line, total_ref, sems.at[halves]))
    copies[-1].start()
    taken = divide(offset - me + devices - 1, devices)
    lane = lax.broadcasted_iota(jnp.int32, (8, span), 1)
    counted = jnp.zeros((8, span), jnp.float32)
    keyed = counted
    for d in range(devices):
        turned = pltpu.roll(recv_ref[d, fields_at : fields_at + 8, :], turns[d], 1)
        other = pltpu.roll(turned, LANES // 2, 1)
        counted = jnp.where(lane >= starts[d], jnp.concatenate([turned] * (span // LANES), 1), counted)
        keyed = jnp.where(lane >= starts[d], jnp.concatenate([other] * (span // LANES), 1), keyed)
    inside = lane[0:1] < taken
    row_line[...] = jnp.where(inside, counted[0:1].astype(jnp.int32), 0)
    key_line[...] = jnp.where(inside, keyed[0:1].astype(jnp.int32), -1)
    for k, (line, goal) in enumerate(((row_line, rows_ref), (key_line, keys_ref))):
        copies.append(pltpu.make_async_copy(line, goal, sems.at[halves + 1 + k]))
        copies[-1].start()
    for copy in copies:
        copy.wait()


def shards(measures, group_index, distinct_keys, group_counts):
    rows, width = measures.shape
    span = distinct_keys.shape[1]
    dims = tuple(lax.axis_size(axis) for axis in AXES)
    devices = dims[0] * dims[1] * dims[2]
    levels = span // devices
    chunks = 4 if rows % (4 * LANES) == 0 else 1
    fields_at = levels * (width // LANES)
    slab = round_up(fields_at + 8, 8)
    wide = round_up(devices, LANES)
    cores = 2 if dims[1] % 2 == 0 else 1
    vmem = pl.BlockSpec(memory_space=pltpu.VMEM)
    smem = pl.BlockSpec(memory_space=pltpu.SMEM)
    anywhere = pl.BlockSpec(memory_space=pl.ANY)
    received, counts = pl.pallas_call(
        functools.partial(
            exchange_kernel, (dims, span, levels, chunks, fields_at)
        ),
        out_shape=(
            pltpu.VMEM((devices, slab, LANES), jnp.float32),
            pltpu.SMEM((1, wide), jnp.int32),
        ),
        in_specs=[anywhere] * 3,
        out_specs=(vmem, smem),
        scratch_shapes=[
            pltpu.VMEM((rows, width), jnp.float32),
            pltpu.VMEM((devices, slab, LANES), jnp.float32),
            pltpu.VMEM((devices, slab, LANES), jnp.float32),
            pltpu.VMEM((span, LANES), jnp.float32),
            pltpu.VMEM((devices // cores, 1, wide), jnp.int32),
            pltpu.VMEM((rows // LANES, LANES), jnp.int32),
            pltpu.VMEM((1, span), jnp.int32),
            pltpu.VMEM((2, 1, wide), jnp.int32),
            pltpu.VMEM((1, wide), jnp.int32),
            pltpu.SemaphoreType.DMA((5,)),
            pltpu.SemaphoreType.DMA((chunks,)),
            pltpu.SemaphoreType.DMA((2,)),
            pltpu.SemaphoreType.DMA((2,)),
        ],
        compiler_params=pltpu.CompilerParams(collective_id=0, has_side_effects=True),
        name="exchange",
    )(group_index.reshape(rows // LANES, LANES), distinct_keys, measures)
    sums, tallies, keys, total = pl.pallas_call(
        functools.partial(place_kernel, (dims, span, levels, fields_at)),
        out_shape=(
            jax.ShapeDtypeStruct((span, width), jnp.float32),
            jax.ShapeDtypeStruct((1, span), jnp.int32),
            jax.ShapeDtypeStruct((1, span), jnp.int32),
            jax.ShapeDtypeStruct((1, 1), jnp.int32),
        ),
        in_specs=[smem, vmem],
        out_specs=(anywhere,) * 4,
        scratch_shapes=[
            pltpu.VMEM((width // LANES, span + round_up(levels, 8), LANES), jnp.float32),
            pltpu.VMEM((1, span), jnp.int32),
            pltpu.VMEM((1, span), jnp.int32),
            pltpu.SMEM((1, 1), jnp.int32),
            pltpu.SemaphoreType.DMA((width // LANES + 3,)),
        ],
        compiler_params=pltpu.CompilerParams(vmem_limit_bytes=16 * 1024 * 1024),
        name="place",
    )(
        pltpu.with_memory_space_constraint(counts, pltpu.SMEM),
        pltpu.with_memory_space_constraint(received, pltpu.VMEM),
    )
    return sums, tallies.reshape(span), keys.reshape(span), total.reshape(())


def solution(mesh):
    return jax.shard_map(
        shards,
        mesh=mesh,
        in_specs=(
            P(AXES, None),
            P(AXES),
            P(AXES, None),
            P(AXES),
        ),
        out_specs=(P(AXES, None), P(AXES), P(AXES), P()),
        check_vma=False,
    )
```

```python
import functools

import jax
import jax.numpy as jnp
from jax import lax
from jax.experimental import pallas as pl
from jax.experimental.pallas import tpu as pltpu
from jax.sharding import PartitionSpec as P

AXES = ("gx", "gy", "gz")
LANES = 128
MESH = pl.DeviceIdType.MESH


def round_up(value, unit):
    return (value + unit - 1) // unit * unit


def wrapped(value, size):
    return jnp.where(value >= size, value - size, value)


def modulo(value, size):
    if size & (size - 1) == 0:
        return value & (size - 1)
    return lax.rem(value, size)


def divide(value, size):
    if size & (size - 1) == 0:
        return lax.shift_right_arithmetic(value, jnp.int32(size.bit_length() - 1))
    return value // size


def flat(spot, dims):
    return (spot[0] * dims[1] + spot[1]) * dims[2] + spot[2]


def targets_of(spots, dims):
    nx, ny, nz = dims
    half = nz // 2 if nz % 2 == 0 else nz
    sides = nz // half
    side = spots[2] // half
    targets = []
    for s in range(1, sides + 1):
        base = wrapped(side + s, sides) * half
        for c in range(half):
            for a in range(nx):
                for b in range(ny):
                    targets.append(((jnp.int32(a), jnp.int32(b), base + c), s == sides))
    return targets


def exchange_kernel(
    shape,
    index_hbm,
    keys_hbm,
    measures_ref,
    recv_ref,
    counts_ref,
    held,
    stage,
    send,
    tally_ref,
    cbuf,
    index_ref,
    keys_ref,
    mate_ref,
    counts_kept,
    small_sem,
    load_sem,
    count_sem,
    data_sem,
    row_sem,
    above_sem,
):
    dims, span, levels, chunks, fields_at = shape
    nx, ny, nz = dims
    devices = nx * ny * nz
    spots = [lax.axis_index(axis) for axis in AXES]
    me = flat(spots, dims)
    ring = [[wrapped(spot + k, size) for k in range(size)] for spot, size in zip(spots, dims)]
    rows, width = held.shape
    chunk = rows // chunks
    halves = width // LANES
    sent_rows = fields_at + 1

    index_load = pltpu.make_async_copy(index_hbm, index_ref, small_sem.at[1])
    index_load.start()
    cores = 2 if ny % 2 == 0 else 1
    core = modulo(spots[1], cores)
    leads = core == cores - 1
    follows = jnp.logical_not(leads)
    pairs = ny // cores
    plane = nx * pairs
    chips = plane * nz
    pair = divide(spots[1], cores)
    level = spots[2]
    chip = level * plane + spots[0] * pairs + pair
    mate = (spots[0], spots[1] + 1 - 2 * core, level)

    def lead(a, b, z):
        return (ring[0][a], wrapped(pair + b, pairs) * cores + cores - 1, z)

    def planes(step, act):
        for c in range(1, nz):
            there = level + step * c
            pl.when(there < nz if step > 0 else there >= 0)(functools.partial(act, there))

    spread = [(a, b) for a in range(nx) for b in range(pairs)]
    barrier = pltpu.get_barrier_semaphore()

    def greet(spot):
        pl.semaphore_signal(barrier, inc=1, device_id=spot, device_id_type=MESH)

    def greet_leads():
        for a, b in spread[1:]:
            greet(lead(a, b, level))
        planes(1, lambda z: [greet(lead(a, b, z)) for a, b in spread] and None)

    if cores == 2:
        greet(mate)
    pl.when(leads)(greet_leads)
    loads = []
    for c in range(chunks):
        piece = pl.ds(c * chunk, chunk)
        load = pltpu.make_async_copy(measures_ref.at[piece], held.at[piece], load_sem.at[c])
        load.start()
        loads.append(load)
    keys_load = pltpu.make_async_copy(keys_hbm, keys_ref, small_sem.at[2])
    keys_load.start()

    def remote(source, goal, send_sem, recv_sem, spot):
        return pltpu.make_async_remote_copy(
            src_ref=source,
            dst_ref=goal,
            send_sem=send_sem,
            recv_sem=recv_sem,
            device_id=tuple(spot),
            device_id_type=MESH,
        )

    def take(ref, sem):
        pltpu.make_async_copy(ref, ref, sem).wait()

    index_load.wait()
    top = jnp.max(index_ref[...], axis=0, keepdims=True)
    mine = jnp.broadcast_to(jnp.max(top, axis=1, keepdims=True) + 1, cbuf.shape[1:])
    lane = lax.broadcasted_iota(jnp.int32, cbuf.shape[1:], 1)
    wide_chip = modulo(lane, nz) * plane + divide(lane, cores * nz)
    wide_core = modulo(divide(lane, nz), cores)

    def tell_mate():
        pl.semaphore_wait(barrier, 1)
        mate_copy.start()

    def tell_leads():
        pl.semaphore_wait(barrier, cores - 1 + plane - 1 + level * plane)
        planes(
            -1,
            lambda z: pl.semaphore_signal(
                above_sem, inc=1, device_id=lead(0, 0, z), device_id_type=MESH
            ),
        )
        if cores == 2:
            mate_copy.wait_recv()
            cbuf[chip] = jnp.where(wide_core == core, mine, mate_ref[1])
        else:
            cbuf[chip] = mine

        def tell(z, some):
            for a, b in some:
                own = cbuf.at[chip]
                remote(own, own, count_sem.at[0], row_sem.at[level], lead(a, b, z)).start()

        tell(level, spread[1:])
        planes(-1, lambda z: tell(z, spread))

    def tell_above():
        if plane > 1:
            take(cbuf.at[pl.ds(0, plane - 1)], row_sem.at[level])
        pl.when(level < nz - 1)(lambda: pl.semaphore_wait(above_sem, nz - 1 - level))
        block = cbuf.at[pl.ds(level * plane, plane)]
        planes(
            1,
            lambda z: remote(
                block, block, count_sem.at[0], row_sem.at[level], lead(0, 0, z)
            ).start(),
        )

    def hear_leads():
        for step in (-1, 1):
            planes(step, lambda z: take(cbuf.at[pl.ds(0, plane)], row_sem.at[z]))
        if cores == 2:
            remote(cbuf, cbuf, count_sem.at[0], count_sem.at[1], mate).start()

    def hear_mate():
        take(cbuf, count_sem.at[1])

    def finish_leads():
        if chips > 1:
            take(cbuf.at[pl.ds(0, chips - 1)], count_sem.at[0])
        if cores == 2:
            take(cbuf, count_sem.at[0])

    if cores == 2:
        mate_ref[0] = mine
        mate_copy = remote(mate_ref.at[0], mate_ref.at[1], small_sem.at[0], small_sem.at[3], mate)
        pl.when(follows)(tell_mate)

    row = lax.broadcasted_iota(jnp.int32, (span, LANES), 0)
    labels = lax.rem(row, levels) * devices + row // levels

    for c in range(chunks):
        loads[c].wait()
        x = held[pl.ds(c * chunk, chunk), :]
        high = x.astype(jnp.bfloat16)
        low = (x - high.astype(jnp.float32)).astype(jnp.bfloat16)
        parts = []
        for j in range(chunk // LANES):
            at = c * (chunk // LANES) + j
            hit = jnp.where(index_ref[pl.ds(at, 1), :] == labels, 1.0, 0.0)
            if at == 0:
                tally_ref[...] = hit
            else:
                tally_ref[...] += hit
            parts.append(hit.astype(jnp.bfloat16))
        hits = jnp.concatenate(parts, axis=1)
        dot = functools.partial(jnp.dot, preferred_element_type=jnp.float32)
        part = dot(hits, high) + dot(hits, low)
        for h in range(halves):
            block = part[:, h * LANES : (h + 1) * LANES].reshape(devices, levels, LANES)
            if c == 0:
                stage[:, h * levels : (h + 1) * levels, :] = block
            else:
                stage[:, h * levels : (h + 1) * levels, :] += block
        if c == 0:
            pl.when(leads)(tell_leads)
    pl.when(leads)(tell_above)

    tallies = lax.dot_general(
        jnp.ones((8, LANES), jnp.bfloat16),
        tally_ref[...].astype(jnp.bfloat16),
        (((1,), (1,)), ((), ())),
        preferred_element_type=jnp.float32,
    )
    keys_load.wait()
    keys = keys_ref[...]
    source = lax.broadcasted_iota(jnp.int32, (span, span), 0)
    goal = lax.broadcasted_iota(jnp.int32, (span, span), 1)
    moved = (source == lax.rem(goal, levels) * devices + goal // levels)
    moved = jnp.where(moved, 1.0, 0.0).astype(jnp.bfloat16)
    line = lax.broadcasted_iota(jnp.int32, (8, span), 0)
    pieces = jnp.where(
        line == 0, keys & 255, jnp.where(line == 1, (keys >> 8) & 255, (keys >> 16) & 255)
    )
    pieces = jnp.dot(
        pieces.astype(jnp.float32).astype(jnp.bfloat16), moved, preferred_element_type=jnp.float32
    )
    placed = pieces[0:1] + pieces[1:2] * 256.0 + pieces[2:3] * 65536.0
    line = lax.broadcasted_iota(jnp.int32, (1, LANES), 1)
    for t in range(span // LANES):
        tile = slice(t * LANES, (t + 1) * LANES)
        keyed = pltpu.roll(jnp.broadcast_to(placed[:, tile], (8, LANES)), LANES // 2, 1)[0:1]
        counted = tallies[0:1, tile]
        lows = jnp.where(line < LANES // 2, counted, keyed)
        highs = jnp.where(line < LANES // 2, keyed, counted)
        for a in range(t * LANES // levels, (t + 1) * LANES // levels):
            within = a * levels % LANES
            stage[a, fields_at : fields_at + 1, :] = lows if within < LANES // 2 else highs

    pl.when(leads)(hear_leads)
    if cores == 2:
        pl.when(follows)(hear_mate)
    shown = cbuf[...][:, 0, :]
    place = lax.broadcasted_iota(jnp.int32, shown.shape, 0)
    counts = jnp.sum(jnp.where(place == wide_chip, shown, 0), axis=0, keepdims=True)
    before = jnp.sum(jnp.where(lane < me, counts, 0))
    shift = modulo(before, devices)

    targets = targets_of(spots, dims)
    piece = pl.ds(0, sent_rows)
    for across in (False, True) if any(not own for _, own in targets) else (True,):
        for spot, own in targets:
            if own == across:
                other = flat(spot, dims)
                send[other] = stage[modulo(other - shift + devices, devices)]
        for spot, own in targets:
            if own == across:
                other = flat(spot, dims)
                copy = remote(
                    send.at[other, piece],
                    recv_ref.at[me, piece],
                    data_sem.at[0],
                    data_sem.at[1],
                    spot,
                )
                if own:
                    pl.when(other != me)(copy.start)
                else:
                    copy.start()
    recv_ref[me] = send[me]
    counts_kept[...] = counts
    counts_copy = pltpu.make_async_copy(counts_kept, counts_ref, small_sem.at[4])
    counts_copy.start()

    pl.when(leads)(finish_leads)
    if cores == 2:
        pl.when(follows)(mate_copy.wait_send)
    landed = recv_ref.at[pl.ds(1, devices - 1), pl.ds(0, sent_rows)]
    left = send.at[pl.ds(1, devices - 1), pl.ds(0, sent_rows)]
    pltpu.make_async_copy(left, left, data_sem.at[0]).wait()
    pltpu.make_async_copy(landed, landed, data_sem.at[1]).wait()
    counts_copy.wait()


def place_kernel(
    shape,
    counts_ref,
    recv_ref,
    sums_ref,
    rows_ref,
    keys_ref,
    total_ref,
    buf,
    row_line,
    key_line,
    total_line,
    sems,
):
    dims, span, levels, fields_at = shape
    nx, ny, nz = dims
    devices = nx * ny * nz
    spots = [lax.axis_index(axis) for axis in AXES]
    me = flat(spots, dims)
    halves = buf.shape[0]

    for h in range(halves):
        buf[h] = jnp.zeros(buf.shape[1:], jnp.float32)
    offset = jnp.int32(0)
    starts, turns = [], []
    for d in range(devices):
        first = modulo(me - modulo(offset, devices) + devices, devices)
        start = divide(offset + first, devices)
        for h in range(halves):
            buf[h, pl.ds(start, levels), :] = recv_ref[d, h * levels : (h + 1) * levels, :]
        starts.append(start)
        turns.append(modulo(start - first * levels + span, LANES))
        offset = offset + counts_ref[0, d]
    copies = []
    for h in range(halves):
        copies.append(
            pltpu.make_async_copy(
                buf.at[h, pl.ds(0, span)], sums_ref.at[:, pl.ds(h * LANES, LANES)], sems.at[h]
            )
        )
        copies[-1].start()

    total_line[0, 0] = offset
    copies.append(pltpu.make_async_copy(total_line, total_ref, sems.at[halves]))
    copies[-1].start()
    taken = divide(offset - me + devices - 1, devices)
    lane = lax.broadcasted_iota(jnp.int32, (8, span), 1)
    counted = jnp.zeros((8, span), jnp.float32)
    keyed = counted
    for d in range(devices):
        turned = pltpu.roll(recv_ref[d, fields_at : fields_at + 8, :], turns[d], 1)
        other = pltpu.roll(turned, LANES // 2, 1)
        counted = jnp.where(lane >= starts[d], jnp.concatenate([turned] * (span // LANES), 1), counted)
        keyed = jnp.where(lane >= starts[d], jnp.concatenate([other] * (span // LANES), 1), keyed)
    inside = lane[0:1] < taken
    row_line[...] = jnp.where(inside, counted[0:1].astype(jnp.int32), 0)
    key_line[...] = jnp.where(inside, keyed[0:1].astype(jnp.int32), -1)
    for k, (line, goal) in enumerate(((row_line, rows_ref), (key_line, keys_ref))):
        copies.append(pltpu.make_async_copy(line, goal, sems.at[halves + 1 + k]))
        copies[-1].start()
    for copy in copies:
        copy.wait()


def shards(measures, group_index, distinct_keys, group_counts):
    rows, width = measures.shape
    span = distinct_keys.shape[1]
    dims = tuple(lax.axis_size(axis) for axis in AXES)
    devices = dims[0] * dims[1] * dims[2]
    levels = span // devices
    chunks = 4 if rows % (4 * LANES) == 0 else 1
    fields_at = levels * (width // LANES)
    slab = round_up(fields_at + 8, 8)
    wide = round_up(devices, LANES)
    cores = 2 if dims[1] % 2 == 0 else 1
    vmem = pl.BlockSpec(memory_space=pltpu.VMEM)
    smem = pl.BlockSpec(memory_space=pltpu.SMEM)
    anywhere = pl.BlockSpec(memory_space=pl.ANY)
    received, counts = pl.pallas_call(
        functools.partial(
            exchange_kernel, (dims, span, levels, chunks, fields_at)
        ),
        out_shape=(
            pltpu.VMEM((devices, slab, LANES), jnp.float32),
            pltpu.SMEM((1, wide), jnp.int32),
        ),
        in_specs=[anywhere] * 3,
        out_specs=(vmem, smem),
        scratch_shapes=[
            pltpu.VMEM((rows, width), jnp.float32),
            pltpu.VMEM((devices, slab, LANES), jnp.float32),
            pltpu.VMEM((devices, slab, LANES), jnp.float32),
            pltpu.VMEM((span, LANES), jnp.float32),
            pltpu.VMEM((devices // cores, 1, wide), jnp.int32),
            pltpu.VMEM((rows // LANES, LANES), jnp.int32),
            pltpu.VMEM((1, span), jnp.int32),
            pltpu.VMEM((2, 1, wide), jnp.int32),
            pltpu.VMEM((1, wide), jnp.int32),
            pltpu.SemaphoreType.DMA((5,)),
            pltpu.SemaphoreType.DMA((chunks,)),
            pltpu.SemaphoreType.DMA((2,)),
            pltpu.SemaphoreType.DMA((2,)),
            pltpu.SemaphoreType.DMA((dims[2],)),
            pltpu.SemaphoreType.REGULAR,
        ],
        compiler_params=pltpu.CompilerParams(collective_id=0, has_side_effects=True),
        name="exchange",
    )(group_index.reshape(rows // LANES, LANES), distinct_keys, measures)
    sums, tallies, keys, total = pl.pallas_call(
        functools.partial(place_kernel, (dims, span, levels, fields_at)),
        out_shape=(
            jax.ShapeDtypeStruct((span, width), jnp.float32),
            jax.ShapeDtypeStruct((1, span), jnp.int32),
            jax.ShapeDtypeStruct((1, span), jnp.int32),
            jax.ShapeDtypeStruct((1, 1), jnp.int32),
        ),
        in_specs=[smem, vmem],
        out_specs=(anywhere,) * 4,
        scratch_shapes=[
            pltpu.VMEM((width // LANES, span + round_up(levels, 8), LANES), jnp.float32),
            pltpu.VMEM((1, span), jnp.int32),
            pltpu.VMEM((1, span), jnp.int32),
            pltpu.SMEM((1, 1), jnp.int32),
            pltpu.SemaphoreType.DMA((width // LANES + 3,)),
        ],
        compiler_params=pltpu.CompilerParams(vmem_limit_bytes=16 * 1024 * 1024),
        name="place",
    )(
        pltpu.with_memory_space_constraint(counts, pltpu.SMEM),
        pltpu.with_memory_space_constraint(received, pltpu.VMEM),
    )
    return sums, tallies.reshape(span), keys.reshape(span), total.reshape(())


def solution(mesh):
    return jax.shard_map(
        shards,
        mesh=mesh,
        in_specs=(
            P(AXES, None),
            P(AXES),
            P(AXES, None),
            P(AXES),
        ),
        out_specs=(P(AXES, None), P(AXES), P(AXES), P()),
        check_vma=False,
    )
```

```python
import functools

import jax
import jax.numpy as jnp
from jax import lax
from jax.experimental import pallas as pl
from jax.experimental.pallas import tpu as pltpu
from jax.sharding import PartitionSpec as P

AXES = ("gx", "gy", "gz")
LANES = 128
MESH = pl.DeviceIdType.MESH


def round_up(value, unit):
    return (value + unit - 1) // unit * unit


def wrapped(value, size):
    return jnp.where(value >= size, value - size, value)


def modulo(value, size):
    if size & (size - 1) == 0:
        return value & (size - 1)
    return lax.rem(value, size)


def divide(value, size):
    if size & (size - 1) == 0:
        return lax.shift_right_arithmetic(value, jnp.int32(size.bit_length() - 1))
    return value // size


def flat(spot, dims):
    return (spot[0] * dims[1] + spot[1]) * dims[2] + spot[2]


def targets_of(spots, dims):
    nx, ny, nz = dims
    half = nz // 2 if nz % 2 == 0 else nz
    sides = nz // half
    side = spots[2] // half
    targets = []
    for s in range(1, sides + 1):
        base = wrapped(side + s, sides) * half
        for c in range(half):
            for a in range(nx):
                for b in range(ny):
                    targets.append(((jnp.int32(a), jnp.int32(b), base + c), s == sides))
    return targets


def exchange_kernel(
    shape,
    index_hbm,
    keys_hbm,
    measures_ref,
    recv_ref,
    counts_ref,
    held,
    stage,
    send,
    tally_ref,
    cbuf,
    index_ref,
    keys_ref,
    mate_ref,
    counts_kept,
    small_sem,
    load_sem,
    count_sem,
    data_sem,
    row_sem,
    above_sem,
):
    dims, span, levels, chunks, fields_at = shape
    nx, ny, nz = dims
    devices = nx * ny * nz
    spots = [lax.axis_index(axis) for axis in AXES]
    me = flat(spots, dims)
    ring = [[wrapped(spot + k, size) for k in range(size)] for spot, size in zip(spots, dims)]
    rows, width = held.shape
    chunk = rows // chunks
    halves = width // LANES
    sent_rows = fields_at + 1

    index_load = pltpu.make_async_copy(index_hbm, index_ref, small_sem.at[1])
    index_load.start()
    cores = 2 if ny % 2 == 0 else 1
    core = modulo(spots[1], cores)
    leads = core == cores - 1
    follows = jnp.logical_not(leads)
    pairs = ny // cores
    plane = nx * pairs
    chips = plane * nz
    pair = divide(spots[1], cores)
    level = spots[2]
    chip = level * plane + spots[0] * pairs + pair
    mate = (spots[0], spots[1] + 1 - 2 * core, level)

    def lead(a, b, z):
        return (ring[0][a], wrapped(pair + b, pairs) * cores + cores - 1, z)

    def planes(step, act):
        for c in range(1, nz):
            there = level + step * c
            pl.when(there < nz if step > 0 else there >= 0)(functools.partial(act, there))

    spread = [(a, b) for a in range(nx) for b in range(pairs)]
    barrier = pltpu.get_barrier_semaphore()

    def greet(spot):
        pl.semaphore_signal(barrier, inc=1, device_id=spot, device_id_type=MESH)

    def greet_leads():
        for a, b in spread[1:]:
            greet(lead(a, b, level))
        planes(1, lambda z: [greet(lead(a, b, z)) for a, b in spread] and None)

    if cores == 2:
        greet(mate)
    pl.when(leads)(greet_leads)
    loads = []
    for c in range(chunks):
        piece = pl.ds(c * chunk, chunk)
        load = pltpu.make_async_copy(measures_ref.at[piece], held.at[piece], load_sem.at[c])
        load.start()
        loads.append(load)
    keys_load = pltpu.make_async_copy(keys_hbm, keys_ref, small_sem.at[2])
    keys_load.start()

    def remote(source, goal, send_sem, recv_sem, spot):
        return pltpu.make_async_remote_copy(
            src_ref=source,
            dst_ref=goal,
            send_sem=send_sem,
            recv_sem=recv_sem,
            device_id=tuple(spot),
            device_id_type=MESH,
        )

    def take(ref, sem):
        pltpu.make_async_copy(ref, ref, sem).wait()

    index_load.wait()
    top = jnp.max(index_ref[...], axis=0, keepdims=True)
    mine = jnp.broadcast_to(jnp.max(top, axis=1, keepdims=True) + 1, cbuf.shape[1:])
    lane = lax.broadcasted_iota(jnp.int32, cbuf.shape[1:], 1)
    wide_chip = modulo(lane, nz) * plane + divide(lane, cores * nz)
    wide_core = modulo(divide(lane, nz), cores)

    def tell_mate():
        pl.semaphore_wait(barrier, 1)
        mate_copy.start()

    def tell_leads():
        pl.semaphore_wait(barrier, cores - 1 + plane - 1 + level * plane)
        planes(
            -1,
            lambda z: pl.semaphore_signal(
                above_sem, inc=1, device_id=lead(0, 0, z), device_id_type=MESH
            ),
        )
        if cores == 2:
            mate_copy.wait_recv()
            cbuf[chip] = jnp.where(wide_core == core, mine, mate_ref[1])
        else:
            cbuf[chip] = mine

        def tell(z, some):
            for a, b in some:
                own = cbuf.at[chip]
                remote(own, own, count_sem.at[0], row_sem.at[level], lead(a, b, z)).start()

        tell(level, spread[1:])
        planes(-1, lambda z: tell(z, spread))

    def tell_above():
        if plane > 1:
            take(cbuf.at[pl.ds(0, plane - 1)], row_sem.at[level])
        pl.when(level < nz - 1)(lambda: pl.semaphore_wait(above_sem, nz - 1 - level))
        block = cbuf.at[pl.ds(level * plane, plane)]
        planes(
            1,
            lambda z: remote(
                block, block, count_sem.at[0], row_sem.at[level], lead(0, 0, z)
            ).start(),
        )

    def hear_leads():
        for step in (-1, 1):
            planes(step, lambda z: take(cbuf.at[pl.ds(0, plane)], row_sem.at[z]))
        if cores == 2:
            remote(cbuf, cbuf, count_sem.at[0], count_sem.at[1], mate).start()

    def hear_mate():
        take(cbuf, count_sem.at[1])

    def finish_leads():
        if chips > 1:
            take(cbuf.at[pl.ds(0, chips - 1)], count_sem.at[0])
        if cores == 2:
            take(cbuf, count_sem.at[0])

    if cores == 2:
        mate_ref[0] = mine
        mate_copy = remote(mate_ref.at[0], mate_ref.at[1], small_sem.at[0], small_sem.at[3], mate)
        pl.when(follows)(tell_mate)

    row = lax.broadcasted_iota(jnp.int32, (span, LANES), 0)
    labels = lax.rem(row, levels) * devices + row // levels

    pl.when(leads)(tell_leads)
    for c in range(chunks):
        loads[c].wait()
        x = held[pl.ds(c * chunk, chunk), :]
        high = x.astype(jnp.bfloat16)
        low = (x - high.astype(jnp.float32)).astype(jnp.bfloat16)
        parts = []
        for j in range(chunk // LANES):
            at = c * (chunk // LANES) + j
            hit = jnp.where(index_ref[pl.ds(at, 1), :] == labels, 1.0, 0.0)
            if at == 0:
                tally_ref[...] = hit
            else:
                tally_ref[...] += hit
            parts.append(hit.astype(jnp.bfloat16))
        hits = jnp.concatenate(parts, axis=1)
        dot = functools.partial(jnp.dot, preferred_element_type=jnp.float32)
        part = dot(hits, high) + dot(hits, low)
        for h in range(halves):
            block = part[:, h * LANES : (h + 1) * LANES].reshape(devices, levels, LANES)
            if c == 0:
                stage[:, h * levels : (h + 1) * levels, :] = block
            else:
                stage[:, h * levels : (h + 1) * levels, :] += block
        if c == -1:
            pl.when(leads)(tell_leads)
        if c == 2:
            pl.when(leads)(tell_above)

    tallies = lax.dot_general(
        jnp.ones((8, LANES), jnp.bfloat16),
        tally_ref[...].astype(jnp.bfloat16),
        (((1,), (1,)), ((), ())),
        preferred_element_type=jnp.float32,
    )
    keys_load.wait()
    keys = keys_ref[...]
    source = lax.broadcasted_iota(jnp.int32, (span, span), 0)
    goal = lax.broadcasted_iota(jnp.int32, (span, span), 1)
    moved = (source == lax.rem(goal, levels) * devices + goal // levels)
    moved = jnp.where(moved, 1.0, 0.0).astype(jnp.bfloat16)
    line = lax.broadcasted_iota(jnp.int32, (8, span), 0)
    pieces = jnp.where(
        line == 0, keys & 255, jnp.where(line == 1, (keys >> 8) & 255, (keys >> 16) & 255)
    )
    pieces = jnp.dot(
        pieces.astype(jnp.float32).astype(jnp.bfloat16), moved, preferred_element_type=jnp.float32
    )
    placed = pieces[0:1] + pieces[1:2] * 256.0 + pieces[2:3] * 65536.0
    line = lax.broadcasted_iota(jnp.int32, (1, LANES), 1)
    for t in range(span // LANES):
        tile = slice(t * LANES, (t + 1) * LANES)
        keyed = pltpu.roll(jnp.broadcast_to(placed[:, tile], (8, LANES)), LANES // 2, 1)[0:1]
        counted = tallies[0:1, tile]
        lows = jnp.where(line < LANES // 2, counted, keyed)
        highs = jnp.where(line < LANES // 2, keyed, counted)
        for a in range(t * LANES // levels, (t + 1) * LANES // levels):
            within = a * levels % LANES
            stage[a, fields_at : fields_at + 1, :] = lows if within < LANES // 2 else highs

    pl.when(leads)(hear_leads)
    if cores == 2:
        pl.when(follows)(hear_mate)
    shown = cbuf[...][:, 0, :]
    place = lax.broadcasted_iota(jnp.int32, shown.shape, 0)
    counts = jnp.sum(jnp.where(place == wide_chip, shown, 0), axis=0, keepdims=True)
    before = jnp.sum(jnp.where(lane < me, counts, 0))
    shift = modulo(before, devices)

    targets = targets_of(spots, dims)
    piece = pl.ds(0, sent_rows)
    for across in (False, True) if any(not own for _, own in targets) else (True,):
        for spot, own in targets:
            if own == across:
                other = flat(spot, dims)
                send[other] = stage[modulo(other - shift + devices, devices)]
        for spot, own in targets:
            if own == across:
                other = flat(spot, dims)
                copy = remote(
                    send.at[other, piece],
                    recv_ref.at[me, piece],
                    data_sem.at[0],
                    data_sem.at[1],
                    spot,
                )
                if own:
                    pl.when(other != me)(copy.start)
                else:
                    copy.start()
    recv_ref[me] = send[me]
    counts_kept[...] = counts
    counts_copy = pltpu.make_async_copy(counts_kept, counts_ref, small_sem.at[4])
    counts_copy.start()

    pl.when(leads)(finish_leads)
    if cores == 2:
        pl.when(follows)(mate_copy.wait_send)
    landed = recv_ref.at[pl.ds(1, devices - 1), pl.ds(0, sent_rows)]
    left = send.at[pl.ds(1, devices - 1), pl.ds(0, sent_rows)]
    pltpu.make_async_copy(left, left, data_sem.at[0]).wait()
    pltpu.make_async_copy(landed, landed, data_sem.at[1]).wait()
    counts_copy.wait()


def place_kernel(
    shape,
    counts_ref,
    recv_ref,
    sums_ref,
    rows_ref,
    keys_ref,
    total_ref,
    buf,
    row_line,
    key_line,
    total_line,
    sems,
):
    dims, span, levels, fields_at = shape
    nx, ny, nz = dims
    devices = nx * ny * nz
    spots = [lax.axis_index(axis) for axis in AXES]
    me = flat(spots, dims)
    halves = buf.shape[0]

    for h in range(halves):
        buf[h] = jnp.zeros(buf.shape[1:], jnp.float32)
    offset = jnp.int32(0)
    starts, turns = [], []
    for d in range(devices):
        first = modulo(me - modulo(offset, devices) + devices, devices)
        start = divide(offset + first, devices)
        for h in range(halves):
            buf[h, pl.ds(start, levels), :] = recv_ref[d, h * levels : (h + 1) * levels, :]
        starts.append(start)
        turns.append(modulo(start - first * levels + span, LANES))
        offset = offset + counts_ref[0, d]
    copies = []
    for h in range(halves):
        copies.append(
            pltpu.make_async_copy(
                buf.at[h, pl.ds(0, span)], sums_ref.at[:, pl.ds(h * LANES, LANES)], sems.at[h]
            )
        )
        copies[-1].start()

    total_line[0, 0] = offset
    copies.append(pltpu.make_async_copy(total_line, total_ref, sems.at[halves]))
    copies[-1].start()
    taken = divide(offset - me + devices - 1, devices)
    lane = lax.broadcasted_iota(jnp.int32, (8, span), 1)
    counted = jnp.zeros((8, span), jnp.float32)
    keyed = counted
    for d in range(devices):
        turned = pltpu.roll(recv_ref[d, fields_at : fields_at + 8, :], turns[d], 1)
        other = pltpu.roll(turned, LANES // 2, 1)
        counted = jnp.where(lane >= starts[d], jnp.concatenate([turned] * (span // LANES), 1), counted)
        keyed = jnp.where(lane >= starts[d], jnp.concatenate([other] * (span // LANES), 1), keyed)
    inside = lane[0:1] < taken
    row_line[...] = jnp.where(inside, counted[0:1].astype(jnp.int32), 0)
    key_line[...] = jnp.where(inside, keyed[0:1].astype(jnp.int32), -1)
    for k, (line, goal) in enumerate(((row_line, rows_ref), (key_line, keys_ref))):
        copies.append(pltpu.make_async_copy(line, goal, sems.at[halves + 1 + k]))
        copies[-1].start()
    for copy in copies:
        copy.wait()


def shards(measures, group_index, distinct_keys, group_counts):
    rows, width = measures.shape
    span = distinct_keys.shape[1]
    dims = tuple(lax.axis_size(axis) for axis in AXES)
    devices = dims[0] * dims[1] * dims[2]
    levels = span // devices
    chunks = 4 if rows % (4 * LANES) == 0 else 1
    fields_at = levels * (width // LANES)
    slab = round_up(fields_at + 8, 8)
    wide = round_up(devices, LANES)
    cores = 2 if dims[1] % 2 == 0 else 1
    vmem = pl.BlockSpec(memory_space=pltpu.VMEM)
    smem = pl.BlockSpec(memory_space=pltpu.SMEM)
    anywhere = pl.BlockSpec(memory_space=pl.ANY)
    received, counts = pl.pallas_call(
        functools.partial(
            exchange_kernel, (dims, span, levels, chunks, fields_at)
        ),
        out_shape=(
            pltpu.VMEM((devices, slab, LANES), jnp.float32),
            pltpu.SMEM((1, wide), jnp.int32),
        ),
        in_specs=[anywhere] * 3,
        out_specs=(vmem, smem),
        scratch_shapes=[
            pltpu.VMEM((rows, width), jnp.float32),
            pltpu.VMEM((devices, slab, LANES), jnp.float32),
            pltpu.VMEM((devices, slab, LANES), jnp.float32),
            pltpu.VMEM((span, LANES), jnp.float32),
            pltpu.VMEM((devices // cores, 1, wide), jnp.int32),
            pltpu.VMEM((rows // LANES, LANES), jnp.int32),
            pltpu.VMEM((1, span), jnp.int32),
            pltpu.VMEM((2, 1, wide), jnp.int32),
            pltpu.VMEM((1, wide), jnp.int32),
            pltpu.SemaphoreType.DMA((5,)),
            pltpu.SemaphoreType.DMA((chunks,)),
            pltpu.SemaphoreType.DMA((2,)),
            pltpu.SemaphoreType.DMA((2,)),
            pltpu.SemaphoreType.DMA((dims[2],)),
            pltpu.SemaphoreType.REGULAR,
        ],
        compiler_params=pltpu.CompilerParams(collective_id=0, has_side_effects=True),
        name="exchange",
    )(group_index.reshape(rows // LANES, LANES), distinct_keys, measures)
    sums, tallies, keys, total = pl.pallas_call(
        functools.partial(place_kernel, (dims, span, levels, fields_at)),
        out_shape=(
            jax.ShapeDtypeStruct((span, width), jnp.float32),
            jax.ShapeDtypeStruct((1, span), jnp.int32),
            jax.ShapeDtypeStruct((1, span), jnp.int32),
            jax.ShapeDtypeStruct((1, 1), jnp.int32),
        ),
        in_specs=[smem, vmem],
        out_specs=(anywhere,) * 4,
        scratch_shapes=[
            pltpu.VMEM((width // LANES, span + round_up(levels, 8), LANES), jnp.float32),
            pltpu.VMEM((1, span), jnp.int32),
            pltpu.VMEM((1, span), jnp.int32),
            pltpu.SMEM((1, 1), jnp.int32),
            pltpu.SemaphoreType.DMA((width // LANES + 3,)),
        ],
        compiler_params=pltpu.CompilerParams(vmem_limit_bytes=16 * 1024 * 1024),
        name="place",
    )(
        pltpu.with_memory_space_constraint(counts, pltpu.SMEM),
        pltpu.with_memory_space_constraint(received, pltpu.VMEM),
    )
    return sums, tallies.reshape(span), keys.reshape(span), total.reshape(())


def solution(mesh):
    return jax.shard_map(
        shards,
        mesh=mesh,
        in_specs=(
            P(AXES, None),
            P(AXES),
            P(AXES, None),
            P(AXES),
        ),
        out_specs=(P(AXES, None), P(AXES), P(AXES), P()),
        check_vma=False,
    )
```

```python
import functools

import jax
import jax.numpy as jnp
from jax import lax
from jax.experimental import pallas as pl
from jax.experimental.pallas import tpu as pltpu
from jax.sharding import PartitionSpec as P

AXES = ("gx", "gy", "gz")
LANES = 128
MESH = pl.DeviceIdType.MESH


def round_up(value, unit):
    return (value + unit - 1) // unit * unit


def wrapped(value, size):
    return jnp.where(value >= size, value - size, value)


def modulo(value, size):
    if size & (size - 1) == 0:
        return value & (size - 1)
    return lax.rem(value, size)


def divide(value, size):
    if size & (size - 1) == 0:
        return lax.shift_right_arithmetic(value, jnp.int32(size.bit_length() - 1))
    return value // size


def flat(spot, dims):
    return (spot[0] * dims[1] + spot[1]) * dims[2] + spot[2]


def targets_of(spots, dims):
    nx, ny, nz = dims
    half = nz // 2 if nz % 2 == 0 else nz
    sides = nz // half
    side = spots[2] // half
    targets = []
    for s in range(1, sides + 1):
        base = wrapped(side + s, sides) * half
        for c in range(half):
            for a in range(nx):
                for b in reversed(range(ny)):
                    targets.append(((jnp.int32(a), jnp.int32(b), base + c), s == sides))
    return targets


def exchange_kernel(
    shape,
    index_hbm,
    keys_hbm,
    measures_ref,
    recv_ref,
    counts_ref,
    held,
    stage,
    send,
    tally_ref,
    cbuf,
    index_ref,
    keys_ref,
    mate_ref,
    counts_kept,
    small_sem,
    load_sem,
    count_sem,
    data_sem,
    row_sem,
    above_sem,
):
    dims, span, levels, chunks, fields_at = shape
    nx, ny, nz = dims
    devices = nx * ny * nz
    spots = [lax.axis_index(axis) for axis in AXES]
    me = flat(spots, dims)
    ring = [[wrapped(spot + k, size) for k in range(size)] for spot, size in zip(spots, dims)]
    rows, width = held.shape
    chunk = rows // chunks
    halves = width // LANES
    sent_rows = fields_at + 1

    index_load = pltpu.make_async_copy(index_hbm, index_ref, small_sem.at[1])
    index_load.start()
    cores = 2 if ny % 2 == 0 else 1
    core = modulo(spots[1], cores)
    leads = core == cores - 1
    follows = jnp.logical_not(leads)
    pairs = ny // cores
    plane = nx * pairs
    chips = plane * nz
    pair = divide(spots[1], cores)
    level = spots[2]
    chip = level * plane + spots[0] * pairs + pair
    mate = (spots[0], spots[1] + 1 - 2 * core, level)

    def lead(a, b, z):
        return (ring[0][a], wrapped(pair + b, pairs) * cores + cores - 1, z)

    def planes(step, act):
        for c in range(1, nz):
            there = level + step * c
            pl.when(there < nz if step > 0 else there >= 0)(functools.partial(act, there))

    spread = [(a, b) for a in range(nx) for b in range(pairs)]
    barrier = pltpu.get_barrier_semaphore()

    def greet(spot):
        pl.semaphore_signal(barrier, inc=1, device_id=spot, device_id_type=MESH)

    def greet_leads():
        for a, b in spread[1:]:
            greet(lead(a, b, level))
        planes(1, lambda z: [greet(lead(a, b, z)) for a, b in spread] and None)

    if cores == 2:
        greet(mate)
    pl.when(leads)(greet_leads)
    loads = []
    for c in range(chunks):
        piece = pl.ds(c * chunk, chunk)
        load = pltpu.make_async_copy(measures_ref.at[piece], held.at[piece], load_sem.at[c])
        load.start()
        loads.append(load)
    keys_load = pltpu.make_async_copy(keys_hbm, keys_ref, small_sem.at[2])
    keys_load.start()

    def remote(source, goal, send_sem, recv_sem, spot):
        return pltpu.make_async_remote_copy(
            src_ref=source,
            dst_ref=goal,
            send_sem=send_sem,
            recv_sem=recv_sem,
            device_id=tuple(spot),
            device_id_type=MESH,
        )

    def take(ref, sem):
        pltpu.make_async_copy(ref, ref, sem).wait()

    index_load.wait()
    top = jnp.max(index_ref[...], axis=0, keepdims=True)
    mine = jnp.broadcast_to(jnp.max(top, axis=1, keepdims=True) + 1, cbuf.shape[1:])
    lane = lax.broadcasted_iota(jnp.int32, cbuf.shape[1:], 1)
    wide_chip = modulo(lane, nz) * plane + divide(lane, cores * nz)
    wide_core = modulo(divide(lane, nz), cores)

    def tell_mate():
        pl.semaphore_wait(barrier, 1)
        mate_copy.start()

    def tell_leads():
        pl.semaphore_wait(barrier, cores - 1 + plane - 1 + level * plane)
        planes(
            -1,
            lambda z: pl.semaphore_signal(
                above_sem, inc=1, device_id=lead(0, 0, z), device_id_type=MESH
            ),
        )
        if cores == 2:
            mate_copy.wait_recv()
            cbuf[chip] = jnp.where(wide_core == core, mine, mate_ref[1])
        else:
            cbuf[chip] = mine

        def tell(z, some):
            for a, b in some:
                own = cbuf.at[chip]
                remote(own, own, count_sem.at[0], row_sem.at[level], lead(a, b, z)).start()

        tell(level, spread[1:])
        planes(-1, lambda z: tell(z, spread))

    def tell_above():
        if plane > 1:
            take(cbuf.at[pl.ds(0, plane - 1)], row_sem.at[level])
        pl.when(level < nz - 1)(lambda: pl.semaphore_wait(above_sem, nz - 1 - level))
        block = cbuf.at[pl.ds(level * plane, plane)]
        planes(
            1,
            lambda z: remote(
                block, block, count_sem.at[0], row_sem.at[level], lead(0, 0, z)
            ).start(),
        )

    def hear_leads():
        for step in (-1, 1):
            planes(step, lambda z: take(cbuf.at[pl.ds(0, plane)], row_sem.at[z]))
        if cores == 2:
            remote(cbuf, cbuf, count_sem.at[0], count_sem.at[1], mate).start()

    def hear_mate():
        take(cbuf, count_sem.at[1])

    def finish_leads():
        if chips > 1:
            take(cbuf.at[pl.ds(0, chips - 1)], count_sem.at[0])
        if cores == 2:
            take(cbuf, count_sem.at[0])

    if cores == 2:
        mate_ref[0] = mine
        mate_copy = remote(mate_ref.at[0], mate_ref.at[1], small_sem.at[0], small_sem.at[3], mate)
        pl.when(follows)(tell_mate)

    row = lax.broadcasted_iota(jnp.int32, (span, LANES), 0)
    labels = lax.rem(row, levels) * devices + row // levels

    pl.when(leads)(tell_leads)
    for c in range(chunks):
        loads[c].wait()
        x = held[pl.ds(c * chunk, chunk), :]
        high = x.astype(jnp.bfloat16)
        low = (x - high.astype(jnp.float32)).astype(jnp.bfloat16)
        parts = []
        for j in range(chunk // LANES):
            at = c * (chunk // LANES) + j
            hit = jnp.where(index_ref[pl.ds(at, 1), :] == labels, 1.0, 0.0)
            if at == 0:
                tally_ref[...] = hit
            else:
                tally_ref[...] += hit
            parts.append(hit.astype(jnp.bfloat16))
        hits = jnp.concatenate(parts, axis=1)
        dot = functools.partial(jnp.dot, preferred_element_type=jnp.float32)
        part = dot(hits, high) + dot(hits, low)
        for h in range(halves):
            block = part[:, h * LANES : (h + 1) * LANES].reshape(devices, levels, LANES)
            if c == 0:
                stage[:, h * levels : (h + 1) * levels, :] = block
            else:
                stage[:, h * levels : (h + 1) * levels, :] += block
        if c == -1:
            pl.when(leads)(tell_leads)
        if c == 2:
            pl.when(leads)(tell_above)

    tallies = lax.dot_general(
        jnp.ones((8, LANES), jnp.bfloat16),
        tally_ref[...].astype(jnp.bfloat16),
        (((1,), (1,)), ((), ())),
        preferred_element_type=jnp.float32,
    )
    keys_load.wait()
    keys = keys_ref[...]
    source = lax.broadcasted_iota(jnp.int32, (span, span), 0)
    goal = lax.broadcasted_iota(jnp.int32, (span, span), 1)
    moved = (source == lax.rem(goal, levels) * devices + goal // levels)
    moved = jnp.where(moved, 1.0, 0.0).astype(jnp.bfloat16)
    line = lax.broadcasted_iota(jnp.int32, (8, span), 0)
    pieces = jnp.where(
        line == 0, keys & 255, jnp.where(line == 1, (keys >> 8) & 255, (keys >> 16) & 255)
    )
    pieces = jnp.dot(
        pieces.astype(jnp.float32).astype(jnp.bfloat16), moved, preferred_element_type=jnp.float32
    )
    placed = pieces[0:1] + pieces[1:2] * 256.0 + pieces[2:3] * 65536.0
    line = lax.broadcasted_iota(jnp.int32, (1, LANES), 1)
    for t in range(span // LANES):
        tile = slice(t * LANES, (t + 1) * LANES)
        keyed = pltpu.roll(jnp.broadcast_to(placed[:, tile], (8, LANES)), LANES // 2, 1)[0:1]
        counted = tallies[0:1, tile]
        lows = jnp.where(line < LANES // 2, counted, keyed)
        highs = jnp.where(line < LANES // 2, keyed, counted)
        for a in range(t * LANES // levels, (t + 1) * LANES // levels):
            within = a * levels % LANES
            stage[a, fields_at : fields_at + 1, :] = lows if within < LANES // 2 else highs

    pl.when(leads)(hear_leads)
    if cores == 2:
        pl.when(follows)(hear_mate)
    shown = cbuf[...][:, 0, :]
    place = lax.broadcasted_iota(jnp.int32, shown.shape, 0)
    counts = jnp.sum(jnp.where(place == wide_chip, shown, 0), axis=0, keepdims=True)
    start_of = (modulo(place, plane) * cores + wide_core) * nz + divide(place, plane)
    ahead = jnp.sum(jnp.where(start_of < me, shown, 0), axis=0, keepdims=True)
    before = ahead[0, 0] + ahead[0, nz] if cores == 2 else ahead[0, 0]
    shift = modulo(before, devices)

    targets = targets_of(spots, dims)
    piece = pl.ds(0, sent_rows)
    far = [target for target in targets if not target[1]]
    near = [target for target in targets if target[1]]
    mixed = far[: len(far) // 2]
    for k, target in enumerate(far[len(far) // 2 :]):
        mixed += [target] + near[2 * k : 2 * k + 2]
    mixed += near[2 * (len(far) - len(far) // 2) :]
    for spot, _ in mixed:
        other = flat(spot, dims)
        send[other] = stage[modulo(other - shift + devices, devices)]
    for spot, own in mixed:
        other = flat(spot, dims)
        copy = remote(
            send.at[other, piece],
            recv_ref.at[me, piece],
            data_sem.at[0],
            data_sem.at[1],
            spot,
        )
        if own:
            pl.when(other != me)(copy.start)
        else:
            copy.start()
    recv_ref[me] = send[me]
    counts_kept[...] = counts
    counts_copy = pltpu.make_async_copy(counts_kept, counts_ref, small_sem.at[4])
    counts_copy.start()

    pl.when(leads)(finish_leads)
    if cores == 2:
        pl.when(follows)(mate_copy.wait_send)
    landed = recv_ref.at[pl.ds(1, devices - 1), pl.ds(0, sent_rows)]
    left = send.at[pl.ds(1, devices - 1), pl.ds(0, sent_rows)]
    pltpu.make_async_copy(left, left, data_sem.at[0]).wait()
    pltpu.make_async_copy(landed, landed, data_sem.at[1]).wait()
    counts_copy.wait()


def place_kernel(
    shape,
    counts_ref,
    recv_ref,
    sums_ref,
    rows_ref,
    keys_ref,
    total_ref,
    buf,
    row_line,
    key_line,
    total_line,
    sems,
):
    dims, span, levels, fields_at = shape
    nx, ny, nz = dims
    devices = nx * ny * nz
    spots = [lax.axis_index(axis) for axis in AXES]
    me = flat(spots, dims)
    halves = buf.shape[0]

    for h in range(halves):
        buf[h] = jnp.zeros(buf.shape[1:], jnp.float32)
    offset = jnp.int32(0)
    starts, turns = [], []
    for d in range(devices):
        first = modulo(me - modulo(offset, devices) + devices, devices)
        starts.append(divide(offset + first, devices))
        turns.append(modulo(starts[d] - first * levels + span, LANES))
        offset = offset + counts_ref[0, d]
    copies = []
    for h in range(halves):
        for d in range(devices):
            buf[h, pl.ds(starts[d], levels), :] = recv_ref[d, h * levels : (h + 1) * levels, :]
        copies.append(
            pltpu.make_async_copy(
                buf.at[h, pl.ds(0, span)], sums_ref.at[:, pl.ds(h * LANES, LANES)], sems.at[h]
            )
        )
        copies[-1].start()

    total_line[0, 0] = offset
    copies.append(pltpu.make_async_copy(total_line, total_ref, sems.at[halves]))
    copies[-1].start()
    taken = divide(offset - me + devices - 1, devices)
    lane = lax.broadcasted_iota(jnp.int32, (8, span), 1)
    counted = jnp.zeros((8, span), jnp.float32)
    keyed = counted
    for d in range(devices):
        turned = pltpu.roll(recv_ref[d, fields_at : fields_at + 8, :], turns[d], 1)
        other = pltpu.roll(turned, LANES // 2, 1)
        counted = jnp.where(lane >= starts[d], jnp.concatenate([turned] * (span // LANES), 1), counted)
        keyed = jnp.where(lane >= starts[d], jnp.concatenate([other] * (span // LANES), 1), keyed)
    inside = lane[0:1] < taken
    row_line[...] = jnp.where(inside, counted[0:1].astype(jnp.int32), 0)
    key_line[...] = jnp.where(inside, keyed[0:1].astype(jnp.int32), -1)
    for k, (line, goal) in enumerate(((row_line, rows_ref), (key_line, keys_ref))):
        copies.append(pltpu.make_async_copy(line, goal, sems.at[halves + 1 + k]))
        copies[-1].start()
    for copy in copies:
        copy.wait()


def shards(measures, group_index, distinct_keys, group_counts):
    rows, width = measures.shape
    span = distinct_keys.shape[1]
    dims = tuple(lax.axis_size(axis) for axis in AXES)
    devices = dims[0] * dims[1] * dims[2]
    levels = span // devices
    chunks = 4 if rows % (4 * LANES) == 0 else 1
    fields_at = levels * (width // LANES)
    slab = round_up(fields_at + 8, 8)
    wide = round_up(devices, LANES)
    cores = 2 if dims[1] % 2 == 0 else 1
    vmem = pl.BlockSpec(memory_space=pltpu.VMEM)
    smem = pl.BlockSpec(memory_space=pltpu.SMEM)
    anywhere = pl.BlockSpec(memory_space=pl.ANY)
    received, counts = pl.pallas_call(
        functools.partial(
            exchange_kernel, (dims, span, levels, chunks, fields_at)
        ),
        out_shape=(
            pltpu.VMEM((devices, slab, LANES), jnp.float32),
            pltpu.SMEM((1, wide), jnp.int32),
        ),
        in_specs=[anywhere] * 3,
        out_specs=(vmem, smem),
        scratch_shapes=[
            pltpu.VMEM((rows, width), jnp.float32),
            pltpu.VMEM((devices, slab, LANES), jnp.float32),
            pltpu.VMEM((devices, slab, LANES), jnp.float32),
            pltpu.VMEM((span, LANES), jnp.float32),
            pltpu.VMEM((devices // cores, 1, wide), jnp.int32),
            pltpu.VMEM((rows // LANES, LANES), jnp.int32),
            pltpu.VMEM((1, span), jnp.int32),
            pltpu.VMEM((2, 1, wide), jnp.int32),
            pltpu.VMEM((1, wide), jnp.int32),
            pltpu.SemaphoreType.DMA((5,)),
            pltpu.SemaphoreType.DMA((chunks,)),
            pltpu.SemaphoreType.DMA((2,)),
            pltpu.SemaphoreType.DMA((2,)),
            pltpu.SemaphoreType.DMA((dims[2],)),
            pltpu.SemaphoreType.REGULAR,
        ],
        compiler_params=pltpu.CompilerParams(collective_id=0, has_side_effects=True),
        name="exchange",
    )(group_index.reshape(rows // LANES, LANES), distinct_keys, measures)
    sums, tallies, keys, total = pl.pallas_call(
        functools.partial(place_kernel, (dims, span, levels, fields_at)),
        out_shape=(
            jax.ShapeDtypeStruct((span, width), jnp.float32),
            jax.ShapeDtypeStruct((1, span), jnp.int32),
            jax.ShapeDtypeStruct((1, span), jnp.int32),
            jax.ShapeDtypeStruct((1, 1), jnp.int32),
        ),
        in_specs=[smem, vmem],
        out_specs=(anywhere,) * 4,
        scratch_shapes=[
            pltpu.VMEM((width // LANES, span + round_up(levels, 8), LANES), jnp.float32),
            pltpu.VMEM((1, span), jnp.int32),
            pltpu.VMEM((1, span), jnp.int32),
            pltpu.SMEM((1, 1), jnp.int32),
            pltpu.SemaphoreType.DMA((width // LANES + 3,)),
        ],
        compiler_params=pltpu.CompilerParams(vmem_limit_bytes=16 * 1024 * 1024),
        name="place",
    )(
        pltpu.with_memory_space_constraint(counts, pltpu.SMEM),
        pltpu.with_memory_space_constraint(received, pltpu.VMEM),
    )
    return sums, tallies.reshape(span), keys.reshape(span), total.reshape(())


def solution(mesh):
    return jax.shard_map(
        shards,
        mesh=mesh,
        in_specs=(
            P(AXES, None),
            P(AXES),
            P(AXES, None),
            P(AXES),
        ),
        out_specs=(P(AXES, None), P(AXES), P(AXES), P()),
        check_vma=False,
    )
```

```python
import functools

import jax
import jax.numpy as jnp
from jax import lax
from jax.experimental import pallas as pl
from jax.experimental.pallas import tpu as pltpu
from jax.sharding import PartitionSpec as P

AXES = ("gx", "gy", "gz")
LANES = 128
MESH = pl.DeviceIdType.MESH


def round_up(value, unit):
    return (value + unit - 1) // unit * unit


def wrapped(value, size):
    return jnp.where(value >= size, value - size, value)


def modulo(value, size):
    if size & (size - 1) == 0:
        return value & (size - 1)
    return lax.rem(value, size)


def divide(value, size):
    if size & (size - 1) == 0:
        return lax.shift_right_arithmetic(value, jnp.int32(size.bit_length() - 1))
    return value // size


def flat(spot, dims):
    return (spot[0] * dims[1] + spot[1]) * dims[2] + spot[2]


def targets_of(spots, dims):
    nx, ny, nz = dims
    half = nz // 2 if nz % 2 == 0 else nz
    sides = nz // half
    side = spots[2] // half
    targets = []
    for s in range(1, sides + 1):
        base = wrapped(side + s, sides) * half
        for c in range(half):
            for a in range(nx):
                for b in reversed(range(ny)):
                    targets.append(((jnp.int32(a), jnp.int32(b), base + c), s == sides))
    return targets


def exchange_kernel(
    shape,
    index_hbm,
    keys_hbm,
    measures_ref,
    recv_ref,
    counts_ref,
    held,
    stage,
    send,
    tally_ref,
    cbuf,
    index_ref,
    keys_ref,
    mate_ref,
    counts_kept,
    small_sem,
    load_sem,
    count_sem,
    data_sem,
    row_sem,
    above_sem,
):
    dims, span, levels, chunks, fields_at = shape
    nx, ny, nz = dims
    devices = nx * ny * nz
    spots = [lax.axis_index(axis) for axis in AXES]
    me = flat(spots, dims)
    ring = [[wrapped(spot + k, size) for k in range(size)] for spot, size in zip(spots, dims)]
    rows, width = held.shape
    chunk = rows // chunks
    halves = width // LANES
    sent_rows = fields_at + 1

    index_load = pltpu.make_async_copy(index_hbm, index_ref, small_sem.at[1])
    index_load.start()
    cores = 2 if ny % 2 == 0 else 1
    core = modulo(spots[1], cores)
    leads = core == cores - 1
    follows = jnp.logical_not(leads)
    pairs = ny // cores
    plane = nx * pairs
    chips = plane * nz
    pair = divide(spots[1], cores)
    level = spots[2]
    chip = level * plane + spots[0] * pairs + pair
    mate = (spots[0], spots[1] + 1 - 2 * core, level)

    def lead(a, b, z):
        return (ring[0][a], wrapped(pair + b, pairs) * cores + cores - 1, z)

    def planes(step, act):
        for c in range(1, nz):
            there = level + step * c
            pl.when(there < nz if step > 0 else there >= 0)(functools.partial(act, there))

    spread = [(a, b) for a in range(nx) for b in range(pairs)]
    barrier = pltpu.get_barrier_semaphore()

    def greet(spot):
        pl.semaphore_signal(barrier, inc=1, device_id=spot, device_id_type=MESH)

    def greet_leads():
        for a, b in spread[1:]:
            greet(lead(a, b, level))
        planes(1, lambda z: [greet(lead(a, b, z)) for a, b in spread] and None)

    if cores == 2:
        greet(mate)
    pl.when(leads)(greet_leads)
    loads = []
    for c in range(chunks):
        piece = pl.ds(c * chunk, chunk)
        load = pltpu.make_async_copy(measures_ref.at[piece], held.at[piece], load_sem.at[c])
        load.start()
        loads.append(load)
    keys_load = pltpu.make_async_copy(keys_hbm, keys_ref, small_sem.at[2])
    keys_load.start()

    def remote(source, goal, send_sem, recv_sem, spot):
        return pltpu.make_async_remote_copy(
            src_ref=source,
            dst_ref=goal,
            send_sem=send_sem,
            recv_sem=recv_sem,
            device_id=tuple(spot),
            device_id_type=MESH,
        )

    def take(ref, sem):
        pltpu.make_async_copy(ref, ref, sem).wait()

    index_load.wait()
    top = jnp.max(index_ref[...], axis=0, keepdims=True)
    mine = jnp.broadcast_to(jnp.max(top, axis=1, keepdims=True) + 1, cbuf.shape[1:])
    lane = lax.broadcasted_iota(jnp.int32, cbuf.shape[1:], 1)
    wide_chip = modulo(lane, nz) * plane + divide(lane, cores * nz)
    wide_core = modulo(divide(lane, nz), cores)

    def tell_mate():
        pl.semaphore_wait(barrier, 1)
        mate_copy.start()

    def tell_leads():
        pl.semaphore_wait(barrier, cores - 1 + plane - 1 + level * plane)
        planes(
            -1,
            lambda z: pl.semaphore_signal(
                above_sem, inc=1, device_id=lead(0, 0, z), device_id_type=MESH
            ),
        )
        if cores == 2:
            mate_copy.wait_recv()
            cbuf[chip] = jnp.where(wide_core == core, mine, mate_ref[1])
        else:
            cbuf[chip] = mine

        def tell(z, some):
            for a, b in some:
                own = cbuf.at[chip]
                remote(own, own, count_sem.at[0], row_sem.at[level], lead(a, b, z)).start()

        tell(level, spread[1:])
        planes(-1, lambda z: tell(z, spread))

    def tell_above():
        if plane > 1:
            take(cbuf.at[pl.ds(0, plane - 1)], row_sem.at[level])
        pl.when(level < nz - 1)(lambda: pl.semaphore_wait(above_sem, nz - 1 - level))
        block = cbuf.at[pl.ds(level * plane, plane)]
        planes(
            1,
            lambda z: remote(
                block, block, count_sem.at[0], row_sem.at[level], lead(0, 0, z)
            ).start(),
        )

    def hear_leads():
        for step in (-1, 1):
            planes(step, lambda z: take(cbuf.at[pl.ds(0, plane)], row_sem.at[z]))
        if cores == 2:
            remote(cbuf, cbuf, count_sem.at[0], count_sem.at[1], mate).start()

    def hear_mate():
        take(cbuf, count_sem.at[1])

    def finish_leads():
        if chips > 1:
            take(cbuf.at[pl.ds(0, chips - 1)], count_sem.at[0])
        if cores == 2:
            take(cbuf, count_sem.at[0])

    if cores == 2:
        mate_ref[0] = mine
        mate_copy = remote(mate_ref.at[0], mate_ref.at[1], small_sem.at[0], small_sem.at[3], mate)
        pl.when(follows)(tell_mate)

    row = lax.broadcasted_iota(jnp.int32, (span, LANES), 0)
    labels = lax.rem(row, levels) * devices + row // levels

    pl.when(leads)(tell_leads)
    for c in range(chunks):
        loads[c].wait()
        x = held[pl.ds(c * chunk, chunk), :]
        high = x.astype(jnp.bfloat16)
        low = (x - high.astype(jnp.float32)).astype(jnp.bfloat16)
        parts = []
        for j in range(chunk // LANES):
            at = c * (chunk // LANES) + j
            hit = jnp.where(index_ref[pl.ds(at, 1), :] == labels, 1.0, 0.0)
            if at == 0:
                tally_ref[...] = hit
            else:
                tally_ref[...] += hit
            parts.append(hit.astype(jnp.bfloat16))
        hits = jnp.concatenate(parts, axis=1)
        dot = functools.partial(jnp.dot, preferred_element_type=jnp.float32)
        part = dot(hits, high) + dot(hits, low)
        for h in range(halves):
            block = part[:, h * LANES : (h + 1) * LANES].reshape(devices, levels, LANES)
            if c == 0:
                stage[:, h * levels : (h + 1) * levels, :] = block
            else:
                stage[:, h * levels : (h + 1) * levels, :] += block
        if c == -1:
            pl.when(leads)(tell_leads)
        if c == min(2, chunks - 1):
            pl.when(leads)(tell_above)

    tallies = lax.dot_general(
        jnp.ones((8, LANES), jnp.bfloat16),
        tally_ref[...].astype(jnp.bfloat16),
        (((1,), (1,)), ((), ())),
        preferred_element_type=jnp.float32,
    )
    keys_load.wait()
    keys = keys_ref[...]
    source = lax.broadcasted_iota(jnp.int32, (span, span), 0)
    goal = lax.broadcasted_iota(jnp.int32, (span, span), 1)
    moved = (source == lax.rem(goal, levels) * devices + goal // levels)
    moved = jnp.where(moved, 1.0, 0.0).astype(jnp.bfloat16)
    line = lax.broadcasted_iota(jnp.int32, (8, span), 0)
    pieces = jnp.where(
        line == 0, keys & 255, jnp.where(line == 1, (keys >> 8) & 255, (keys >> 16) & 255)
    )
    pieces = jnp.dot(
        pieces.astype(jnp.float32).astype(jnp.bfloat16), moved, preferred_element_type=jnp.float32
    )
    placed = pieces[0:1] + pieces[1:2] * 256.0 + pieces[2:3] * 65536.0
    line = lax.broadcasted_iota(jnp.int32, (1, LANES), 1)
    for t in range(span // LANES):
        tile = slice(t * LANES, (t + 1) * LANES)
        keyed = pltpu.roll(jnp.broadcast_to(placed[:, tile], (8, LANES)), LANES // 2, 1)[0:1]
        counted = tallies[0:1, tile]
        lows = jnp.where(line < LANES // 2, counted, keyed)
        highs = jnp.where(line < LANES // 2, keyed, counted)
        for a in range(t * LANES // levels, (t + 1) * LANES // levels):
            within = a * levels % LANES
            stage[a, fields_at : fields_at + 1, :] = lows if within < LANES // 2 else highs

    pl.when(leads)(hear_leads)
    if cores == 2:
        pl.when(follows)(hear_mate)
    shown = cbuf[...][:, 0, :]
    place = lax.broadcasted_iota(jnp.int32, shown.shape, 0)
    counts = jnp.sum(jnp.where(place == wide_chip, shown, 0), axis=0, keepdims=True)
    start_of = (modulo(place, plane) * cores + wide_core) * nz + divide(place, plane)
    ahead = jnp.sum(jnp.where(start_of < me, shown, 0), axis=0, keepdims=True)
    before = ahead[0, 0] + ahead[0, nz] if cores == 2 else ahead[0, 0]
    shift = modulo(before, devices)

    targets = targets_of(spots, dims)
    piece = pl.ds(0, sent_rows)
    far = [target for target in targets if not target[1]]
    near = [target for target in targets if target[1]]
    mixed = far[: len(far) // 2]
    for k, target in enumerate(far[len(far) // 2 :]):
        mixed += [target] + near[2 * k : 2 * k + 2]
    mixed += near[2 * (len(far) - len(far) // 2) :]
    for spot, _ in mixed:
        other = flat(spot, dims)
        send[other] = stage[modulo(other - shift + devices, devices)]
    for spot, own in mixed:
        other = flat(spot, dims)
        copy = remote(
            send.at[other, piece],
            recv_ref.at[me, piece],
            data_sem.at[0],
            data_sem.at[1],
            spot,
        )
        if own:
            pl.when(other != me)(copy.start)
        else:
            copy.start()
    recv_ref[me] = send[me]
    counts_kept[...] = counts
    counts_copy = pltpu.make_async_copy(counts_kept, counts_ref, small_sem.at[4])
    counts_copy.start()

    pl.when(leads)(finish_leads)
    if cores == 2:
        pl.when(follows)(mate_copy.wait_send)
    landed = recv_ref.at[pl.ds(1, devices - 1), pl.ds(0, sent_rows)]
    left = send.at[pl.ds(1, devices - 1), pl.ds(0, sent_rows)]
    pltpu.make_async_copy(left, left, data_sem.at[0]).wait()
    pltpu.make_async_copy(landed, landed, data_sem.at[1]).wait()
    counts_copy.wait()


def place_kernel(
    shape,
    counts_ref,
    recv_ref,
    sums_ref,
    rows_ref,
    keys_ref,
    total_ref,
    buf,
    row_line,
    key_line,
    total_line,
    sems,
):
    dims, span, levels, fields_at = shape
    nx, ny, nz = dims
    devices = nx * ny * nz
    spots = [lax.axis_index(axis) for axis in AXES]
    me = flat(spots, dims)
    halves = buf.shape[0]

    for h in range(halves):
        buf[h] = jnp.zeros(buf.shape[1:], jnp.float32)
    offset = jnp.int32(0)
    starts, turns = [], []
    for d in range(devices):
        first = modulo(me - modulo(offset, devices) + devices, devices)
        starts.append(divide(offset + first, devices))
        turns.append(modulo(starts[d] - first * levels + span, LANES))
        offset = offset + counts_ref[0, d]
    copies = []
    for h in range(halves):
        for d in range(devices):
            buf[h, pl.ds(starts[d], levels), :] = recv_ref[d, h * levels : (h + 1) * levels, :]
        copies.append(
            pltpu.make_async_copy(
                buf.at[h, pl.ds(0, span)], sums_ref.at[:, pl.ds(h * LANES, LANES)], sems.at[h]
            )
        )
        copies[-1].start()

    total_line[0, 0] = offset
    copies.append(pltpu.make_async_copy(total_line, total_ref, sems.at[halves]))
    copies[-1].start()
    taken = divide(offset - me + devices - 1, devices)
    lane = lax.broadcasted_iota(jnp.int32, (8, span), 1)
    counted = jnp.zeros((8, span), jnp.float32)
    keyed = counted
    for d in range(devices):
        turned = pltpu.roll(recv_ref[d, fields_at : fields_at + 8, :], turns[d], 1)
        other = pltpu.roll(turned, LANES // 2, 1)
        counted = jnp.where(lane >= starts[d], jnp.concatenate([turned] * (span // LANES), 1), counted)
        keyed = jnp.where(lane >= starts[d], jnp.concatenate([other] * (span // LANES), 1), keyed)
    inside = lane[0:1] < taken
    row_line[...] = jnp.where(inside, counted[0:1].astype(jnp.int32), 0)
    key_line[...] = jnp.where(inside, keyed[0:1].astype(jnp.int32), -1)
    for k, (line, goal) in enumerate(((row_line, rows_ref), (key_line, keys_ref))):
        copies.append(pltpu.make_async_copy(line, goal, sems.at[halves + 1 + k]))
        copies[-1].start()
    for copy in copies:
        copy.wait()


def shards(measures, group_index, distinct_keys, group_counts):
    rows, width = measures.shape
    span = distinct_keys.shape[1]
    dims = tuple(lax.axis_size(axis) for axis in AXES)
    devices = dims[0] * dims[1] * dims[2]
    levels = span // devices
    chunks = 4 if rows % (4 * LANES) == 0 else 1
    fields_at = levels * (width // LANES)
    slab = round_up(fields_at + 8, 8)
    wide = round_up(devices, LANES)
    cores = 2 if dims[1] % 2 == 0 else 1
    vmem = pl.BlockSpec(memory_space=pltpu.VMEM)
    smem = pl.BlockSpec(memory_space=pltpu.SMEM)
    anywhere = pl.BlockSpec(memory_space=pl.ANY)
    received, counts = pl.pallas_call(
        functools.partial(
            exchange_kernel, (dims, span, levels, chunks, fields_at)
        ),
        out_shape=(
            pltpu.VMEM((devices, slab, LANES), jnp.float32),
            pltpu.SMEM((1, wide), jnp.int32),
        ),
        in_specs=[anywhere] * 3,
        out_specs=(vmem, smem),
        scratch_shapes=[
            pltpu.VMEM((rows, width), jnp.float32),
            pltpu.VMEM((devices, slab, LANES), jnp.float32),
            pltpu.VMEM((devices, slab, LANES), jnp.float32),
            pltpu.VMEM((span, LANES), jnp.float32),
            pltpu.VMEM((devices // cores, 1, wide), jnp.int32),
            pltpu.VMEM((rows // LANES, LANES), jnp.int32),
            pltpu.VMEM((1, span), jnp.int32),
            pltpu.VMEM((2, 1, wide), jnp.int32),
            pltpu.VMEM((1, wide), jnp.int32),
            pltpu.SemaphoreType.DMA((5,)),
            pltpu.SemaphoreType.DMA((chunks,)),
            pltpu.SemaphoreType.DMA((2,)),
            pltpu.SemaphoreType.DMA((2,)),
            pltpu.SemaphoreType.DMA((dims[2],)),
            pltpu.SemaphoreType.REGULAR,
        ],
        compiler_params=pltpu.CompilerParams(collective_id=0, has_side_effects=True),
        name="exchange",
    )(group_index.reshape(rows // LANES, LANES), distinct_keys, measures)
    sums, tallies, keys, total = pl.pallas_call(
        functools.partial(place_kernel, (dims, span, levels, fields_at)),
        out_shape=(
            jax.ShapeDtypeStruct((span, width), jnp.float32),
            jax.ShapeDtypeStruct((1, span), jnp.int32),
            jax.ShapeDtypeStruct((1, span), jnp.int32),
            jax.ShapeDtypeStruct((1, 1), jnp.int32),
        ),
        in_specs=[smem, vmem],
        out_specs=(anywhere,) * 4,
        scratch_shapes=[
            pltpu.VMEM((width // LANES, span + round_up(levels, 8), LANES), jnp.float32),
            pltpu.VMEM((1, span), jnp.int32),
            pltpu.VMEM((1, span), jnp.int32),
            pltpu.SMEM((1, 1), jnp.int32),
            pltpu.SemaphoreType.DMA((width // LANES + 3,)),
        ],
        compiler_params=pltpu.CompilerParams(vmem_limit_bytes=16 * 1024 * 1024),
        name="place",
    )(
        pltpu.with_memory_space_constraint(counts, pltpu.SMEM),
        pltpu.with_memory_space_constraint(received, pltpu.VMEM),
    )
    return sums, tallies.reshape(span), keys.reshape(span), total.reshape(())


def solution(mesh):
    return jax.shard_map(
        shards,
        mesh=mesh,
        in_specs=(
            P(AXES, None),
            P(AXES),
            P(AXES, None),
            P(AXES),
        ),
        out_specs=(P(AXES, None), P(AXES), P(AXES), P()),
        check_vma=False,
    )
```
